64 devices in a mesh: stage: 4 (over x, y), data: 16 (over z, core).
Axes of the slice: x: 2, y: 2, z: 8, core: 2. Of those that a mesh axis runs over, the one named last changes fastest.
The devices are a block of a 4x4x8 slice.
Arguments:
- grad_attn: float32 [64, 1, 1536, 1536], P(('stage', 'data')), parts along dimension 0
- mom_attn: float32 [4, 1536, 1536], P('stage', 'data'), parts along dimension 0
- master_attn: float32 [4, 1536, 1536], P('stage', 'data'), parts along dimension 0
- grad_up: float32 [64, 1, 1536, 512], P(('stage', 'data')), parts along dimension 0
- mom_up: float32 [4, 1536, 512], P('stage', 'data'), parts along dimension 0
- master_up: float32 [4, 1536, 512], P('stage', 'data'), parts along dimension 0
- grad_down: float32 [64, 1, 512, 1536], P(('stage', 'data')), parts along dimension 0
- mom_down: float32 [4, 512, 1536], P('stage', 'data'), parts along dimension 0
- master_down: float32 [4, 512, 1536], P('stage', 'data'), parts along dimension 0
Outputs:
- output 1: float32 [4, 1536, 1536], P('stage', 'data'), parts along dimension 0
- output 2: float32 [4, 1536, 1536], P('stage', 'data'), parts along dimension 0
- output 3: bfloat16 [4, 1536, 1536], P('stage', 'data'), parts along dimension 0
- output 4: float32 [4, 1536, 512], P('stage', 'data'), parts along dimension 0
- output 5: float32 [4, 1536, 512], P('stage', 'data'), parts along dimension 0
- output 6: bfloat16 [4, 1536, 512], P('stage', 'data'), parts along dimension 0
- output 7: float32 [4, 512, 1536], P('stage', 'data'), parts along dimension 0
- output 8: float32 [4, 512, 1536], P('stage', 'data'), parts along dimension 0
- output 9: bfloat16 [4, 512, 1536], P('stage', 'data'), parts along dimension 0
There are 4 independent parts. The reference program is written for one: setup_inputs(seed, part) draws one part's arguments, and reference() takes and returns one part's arrays. A program takes and returns all parts, laid end to end along the dimension named above; each array names one.
All inputs are finite; a program needn't handle non-finite values.
Results may differ from the reference program's by a relative error of at most 0.00769194.
Values are sent between devices in bfloat16 or wider.
A program may use at most 768 MiB of HBM per device.

```python
import math
import jax
import jax.numpy as jnp
from jax import lax

HIDDEN = 1536
FFN_WIDTH = 512
ATTN_COUNT = 1
EXPERT_COUNT = 1
GROUP_SIZE = 16
NS_STEPS = 5

MOMENTUM = 0.95
LEARN_RATE = 0.25
WEIGHT_DECAY = 0.2
EPSILON = 1e-7
COEF_A = 3.4445
COEF_B = -4.7750
COEF_C = 2.0315
STACK_SHAPES = ((ATTN_COUNT, HIDDEN, HIDDEN), (EXPERT_COUNT, HIDDEN, FFN_WIDTH), (EXPERT_COUNT, FFN_WIDTH, HIDDEN))
STACK_NAMES = ('attn', 'up', 'down')


def draw_grads(key, count, n_rows, n_cols):
    noise = jax.random.normal(key, (GROUP_SIZE, count, n_rows, n_cols), jnp.float32)
    row_owner = jnp.arange(n_rows) // (n_rows // GROUP_SIZE)
    scale = jnp.where(row_owner[None, :] == jnp.arange(GROUP_SIZE)[:, None], 0.8 * GROUP_SIZE, 0.5)
    return noise * scale[:, None, :, None]


def setup_inputs(seed: int = 0, part: int = 0) -> dict:
    base_key = jax.random.fold_in(jax.random.key(seed), part)
    keys = jax.random.split(base_key, 9)
    inputs = {}
    for stack_idx in range(3):
        count, n_rows, n_cols = STACK_SHAPES[stack_idx]
        label = STACK_NAMES[stack_idx]
        inputs['grad_' + label] = draw_grads(keys[3 * stack_idx], count, n_rows, n_cols)
        inputs['mom_' + label] = jax.random.normal(keys[3 * stack_idx + 1], (count, n_rows, n_cols), jnp.float32)
        inputs['master_' + label] = 0.5 * jax.random.normal(keys[3 * stack_idx + 2], (count, n_rows, n_cols), jnp.float32)
    return inputs


def orthogonalize(mom_new):
    n_rows, n_cols = mom_new.shape
    norm = jnp.sqrt(jnp.sum(mom_new * mom_new))
    x_mat = (mom_new / (norm + EPSILON)).astype(jnp.bfloat16)
    if n_rows > n_cols:
        x_mat = x_mat.T
    for _ in range(NS_STEPS):
        gram_mat = jnp.dot(x_mat, x_mat.T, preferred_element_type=jnp.float32).astype(jnp.bfloat16)
        gram_sq = jnp.dot(gram_mat, gram_mat, preferred_element_type=jnp.float32).astype(jnp.bfloat16)
        poly_mat = (COEF_B * gram_mat.astype(jnp.float32) + COEF_C * gram_sq.astype(jnp.float32)).astype(jnp.bfloat16)
        update = jnp.dot(poly_mat, x_mat, preferred_element_type=jnp.float32).astype(jnp.bfloat16)
        x_mat = (COEF_A * x_mat.astype(jnp.float32) + update.astype(jnp.float32)).astype(jnp.bfloat16)
    if n_rows > n_cols:
        x_mat = x_mat.T
    return x_mat


def stack_step(grad_all, mom_old, master_old):
    n_rows, n_cols = mom_old.shape[1], mom_old.shape[2]
    grad_mean = jnp.sum(grad_all, axis=0) / GROUP_SIZE
    mom_new = MOMENTUM * mom_old + grad_mean
    ortho_mat = lax.map(orthogonalize, mom_new)
    scale = 0.2 * math.sqrt(max(n_rows, n_cols))
    master_new = master_old - LEARN_RATE * (scale * ortho_mat.astype(jnp.float32) + WEIGHT_DECAY * master_old)
    return mom_new, master_new, master_new.astype(jnp.bfloat16)


def reference(grad_attn, mom_attn, master_attn, grad_up, mom_up, master_up, grad_down, mom_down, master_down):
    attn_out = stack_step(grad_attn, mom_attn, master_attn)
    up_out = stack_step(grad_up, mom_up, master_up)
    down_out = stack_step(grad_down, mom_down, master_down)
    return (attn_out[0], attn_out[1], attn_out[2], up_out[0], up_out[1], up_out[2], down_out[0], down_out[1], down_out[2])
```

```python
import functools
import math
import jax
import jax.numpy as jnp
from jax import lax
from jax.experimental import pallas as pl
from jax.experimental.pallas import tpu as pltpu
from jax.sharding import PartitionSpec as P

MOMENTUM = 0.95
LEARN_RATE = 0.25
WEIGHT_DECAY = 0.2
EPSILON = 1e-7
COEF_A = 3.4445
COEF_B = -4.7750
COEF_C = 2.0315
NS_STEPS = 5
F32 = jnp.float32
BF16 = jnp.bfloat16


def dot_nn(a, b):
    return lax.dot_general(a, b, (((1,), (0,)), ((), ())), preferred_element_type=F32)


def dot_nt(a, b):
    return lax.dot_general(a, b, (((1,), (1,)), ((), ())), preferred_element_type=F32)


def remote(src, dst, send_sem, recv_sem, dev):
    return pltpu.make_async_remote_copy(
        src_ref=src, dst_ref=dst, send_sem=send_sem, recv_sem=recv_sem,
        device_id={'data': dev}, device_id_type=pl.DeviceIdType.MESH)


def ds(start, size, mult):
    return pl.ds(pl.multiple_of(start, mult), size)


class Place:
    def __init__(self, group):
        self.group = group
        self.chips = group // 2
        self.me = lax.axis_index('data')
        self.chip = self.me // 2
        self.core = self.me % 2
        self.partner = self.chip * 2 + (1 - self.core)

    def at(self, offset):
        return lax.rem(self.chip + offset + self.chips, self.chips)

    def next(self, way):
        return self.at(1 if way == 0 else -1) * 2 + self.core


class Scatter:
    def __init__(self, place, grad, own, pair, ring, load, psend, precv, rsend, rrecv):
        self.pl, self.grad, self.own, self.pair, self.ring = place, grad, own, pair, ring
        self.load, self.psend, self.precv, self.rsend, self.rrecv = load, psend, precv, rsend, rrecv
        self.rows = own.shape[1]
        self.half_rows = self.rows // 2
        self.n = place.chips
        self.pieces = self.n - 1

    def order(self):
        far = self.n // 2
        order = [far]
        for d in range(far - 1, 0, -1):
            order += [d, self.n - d]
        return order + [0]

    def load_copy(self, d):
        row = (self.pl.at(d) * 2 + self.pl.core) * self.rows
        return pltpu.make_async_copy(self.grad.at[ds(row, self.rows, 32), :], self.own.at[d], self.load.at[d])

    def pair_copy(self, d):
        row = (self.pl.at(d) * 2 + (1 - self.pl.core)) * self.rows
        return remote(self.grad.at[ds(row, self.rows, 32), :], self.pair.at[d], self.psend.at[d], self.precv.at[d], self.pl.partner)

    def start(self):
        for d in self.order():
            self.pair_copy(d).start()
            self.load_copy(d).start()

    def arrive(self, d):
        self.load_copy(d).wait()
        self.pair_copy(d).wait_recv()

    def spot(self, way, q):
        dist = self.n // 2 - (q + 1) // 2
        half = way if q % 2 == 0 else 1 - way
        return dist, (dist if way == 0 else (self.n - dist) % self.n), pl.ds(half * self.half_rows, self.half_rows)

    def ring_copy(self, way, q):
        dist, d, rows = self.spot(way, q)
        return remote(self.own.at[d, rows, :], self.ring.at[way, dist - 1, rows, :], self.rsend.at[way, q], self.rrecv.at[way, q], self.pl.next(way))

    def step(self, q):
        for way in (0, 1):
            dist, d, rows = self.spot(way, q)
            if q % 2 == 1 or (q == 0 and way == 0):
                self.arrive(d)
            total = self.own[d, rows, :] + self.pair[d, rows, :]
            if q >= 2:
                self.ring_copy(way, q - 2).wait_recv()
                total = total + self.ring[way, dist, rows, :]
            self.own[d, rows, :] = total
            self.ring_copy(way, q).start()

    def total(self):
        self.arrive(0)
        for way in (0, 1):
            for q in (self.pieces - 2, self.pieces - 1):
                self.ring_copy(way, q).wait_recv()
        return (self.own[0] + self.pair[0]) + (self.ring[0, 0] + self.ring[1, 0])

    def drain(self):
        for d in range(self.n):
            self.pair_copy(d).wait_send()
        for way in (0, 1):
            for q in range(self.pieces):
                self.ring_copy(way, q).wait_send()


class Gather:
    def __init__(self, place, full, rows, rsend, rrecv, fsend, frecv):
        self.pl, self.full, self.rows = place, full, rows
        self.rsend, self.rrecv, self.fsend, self.frecv = rsend, rrecv, fsend, frecv
        self.half_rows = rows // 2
        self.n = place.chips
        self.pieces = self.n - 1

    def piece(self, way, q, core, lag):
        hop = q // 2 + lag
        chip = self.pl.at(-hop if way == 0 else hop)
        half = way if q % 2 == 0 else 1 - way
        row = (chip * 2 + core) * self.rows + half * self.half_rows
        return self.full.at[ds(row, self.half_rows, 16), :]

    def ring_copy(self, way, q):
        ref = self.piece(way, q, self.pl.core, 0)
        return remote(ref, ref, self.rsend.at[way, q], self.rrecv.at[way, q], self.pl.next(way))

    def arrival(self, way, q):
        ref = self.piece(way, q, self.pl.core, 1)
        return remote(ref, ref, self.rsend.at[way, q], self.rrecv.at[way, q], self.pl.next(way))

    def forward(self, way, q, core):
        ref = self.piece(way, q, core, 1)
        return remote(ref, ref, self.fsend.at[way, q], self.frecv.at[way, q], self.pl.partner)

    def own_rows(self, core):
        return self.full.at[ds((self.pl.chip * 2 + core) * self.rows, self.rows, 32), :]

    def forward_own(self, core):
        ref = self.own_rows(core)
        return remote(ref, ref, self.fsend.at[0, self.pieces], self.frecv.at[0, self.pieces], self.pl.partner)

    def step(self, q):
        if q == 0:
            for k in (0, 1):
                for way in (0, 1):
                    self.ring_copy(way, k).start()
            self.forward_own(self.pl.core).start()
        else:
            for way in (0, 1):
                self.arrival(way, q - 1).wait_recv()
                if q + 1 < self.pieces:
                    self.ring_copy(way, q + 1).start()
                self.forward(way, q - 1, self.pl.core).start()

    def steps(self):
        return self.pieces + 1

    def finish(self):
        self.forward_own(1 - self.pl.core).wait_recv()
        for way in (0, 1):
            for q in range(self.pieces):
                self.forward(way, q, 1 - self.pl.core).wait_recv()

    def drain(self):
        self.forward_own(self.pl.core).wait_send()
        for way in (0, 1):
            for q in range(self.pieces):
                self.forward(way, q, self.pl.core).wait_send()
                self.ring_copy(way, q).wait_send()


def squares(mat):
    sq = mat * mat
    rows, cols = mat.shape
    acc = sq[0:8]
    for i in range(1, rows // 8):
        acc = acc + sq[8 * i:8 * i + 8]
    out = acc[:, 0:128]
    for j in range(1, cols // 128):
        out = out + acc[:, 128 * j:128 * j + 128]
    return out


def total_norm(ref, top):
    acc = ref[0, top:top + 8]
    for i in range(1, ref.shape[0]):
        acc = acc + ref[i, top:top + 8]
    total = jnp.sum(jnp.sum(acc, axis=1, keepdims=True), axis=0, keepdims=True)
    return jnp.sqrt(total) + EPSILON


def kernel(group, grads, moms, masters, outs, sc):
    place = Place(group)
    core, chip = place.core, place.chip
    chips = place.chips
    pieces = chips - 1
    barrier = pltpu.get_barrier_semaphore()
    for dev in (place.partner, place.next(0), place.next(1)):
        pl.semaphore_signal(barrier, inc=1, device_id={'data': dev}, device_id_type=pl.DeviceIdType.MESH)
    pl.semaphore_wait(barrier, 3)

    scat = [Scatter(place, grads[k], sc['own'][k], sc['pair'][k], sc['ring'][k], sc['load'].at[k], sc['psend'].at[k], sc['precv'].at[k],
                    sc['rsend'].at[k], sc['rrecv'].at[k]) for k in range(3)]
    fulls = [sc['x'].at[0], sc['tall'], sc['xu'].at[0]]
    gath = [Gather(place, fulls[k], sc['own'][k].shape[1], sc['gsend'].at[k], sc['grecv'].at[k], sc['fsend'].at[k], sc['frecv'].at[k]) for k in range(3)]

    scat[0].start()
    in_copies = []
    for k in range(3):
        in_copies.append((pltpu.make_async_copy(moms[k], sc['mom'][k], sc['insem'].at[k]),
                          pltpu.make_async_copy(masters[k], sc['master'][k], sc['insem'].at[3 + k])))
    for pair in in_copies:
        for copy in pair:
            copy.start()
    scat[1].start()
    scat[2].start()

    def out_copy(k, j, ref):
        return pltpu.make_async_copy(ref, outs[3 * k + j], sc['outsem'].at[3 * k + j])

    def momentum(k):
        in_copies[k][0].wait()
        mat = MOMENTUM * sc['mom'][k][...] + scat[k].total() * (1.0 / group)
        sc['mom'][k][...] = mat
        out_copy(k, 0, sc['mom'][k]).start()
        return squares(mat)

    def norm_copy(idx, i):
        ref = sc['norm'][idx]
        dev = lax.rem(place.me + i, group)
        return remote(ref.at[0], ref.at[i], sc['nsend'].at[idx, i], sc['nrecv'].at[idx, i], dev)

    def norm_send(idx):
        for i in range(1, group):
            norm_copy(idx, i).start()

    def norm_wait(idx):
        for i in range(1, group):
            norm_copy(idx, i).wait_recv()

    def norm_drain(idx):
        for i in range(1, group):
            norm_copy(idx, i).wait_send()

    def write_x(k, norm):
        rows = sc['own'][k].shape[1]
        fulls[k][ds((chip * 2 + core) * rows, rows, 32), :] = (sc['mom'][k][...] / norm).astype(BF16)

    for q in range(pieces):
        scat[0].step(q)
    sc['norm'][0][0] = momentum(0)
    norm_send(0)
    for q in (0, 1):
        for k in (1, 2):
            scat[k].step(q)
    norm_wait(0)
    write_x(0, total_norm(sc['norm'][0], 0))
    for q in range(gath[0].steps()):
        gath[0].step(q)
    gath[0].finish()

    tasks = {}

    def background(it, slot, fn):
        tasks.setdefault((it, slot), []).append(fn)

    def ud_momentum():
        sc['norm'][1][0, 0:8] = momentum(1)
        sc['norm'][1][0, 8:16] = momentum(2)
        norm_send(1)

    def ud_write():
        norm_wait(1)
        write_x(1, total_norm(sc['norm'][1], 0))
        write_x(2, total_norm(sc['norm'][1], 8))

    def both(parts, q):
        def run():
            parts[1].step(q)
            parts[2].step(q)
        return run

    background(0, 1, gath[0].drain)
    times = [(0, 3), (0, 5), (1, 1), (1, 3), (1, 5)]
    for q in range(2, pieces):
        background(*times[q - 2], both(scat, q))
    background(2, 0, ud_momentum)
    background(2, 1, ud_write)
    times = [(2, 1), (2, 2), (2, 3), (2, 4), (3, 0), (3, 2), (3, 3), (3, 4)]
    for q in range(gath[1].steps()):
        background(*times[q], both(gath, q))

    x, a, b, qacc = sc['x'], sc['a'], sc['b'], sc['qacc']
    size = x.shape[1]
    half = size // 2
    mine = ds(core * half, half, 128)
    theirs = ds((1 - core) * half, half, 128)

    def a_copy(i):
        if i == 0:
            return remote(a.at[mine, mine], a.at[mine, mine], sc['asend'].at[0], sc['arecv'].at[0], place.partner)
        rows = ds(core * half + (i - 1) * (half // 2), half // 2, 128)
        return remote(a.at[rows, theirs], a.at[rows, theirs], sc['asend'].at[i], sc['arecv'].at[i], place.partner)

    def x_copy(buf, n):
        ref = x.at[buf, mine, pl.ds(n * half, half)]
        return remote(ref, ref, sc['xsend'].at[n], sc['xrecv'].at[n], place.partner)

    def ns_step(it, carry):
        cur = lax.rem(it, 2)
        nxt = 1 - cur

        def slot(s):
            for (t, u), fns in tasks.items():
                if u == s:
                    def run(fns=fns):
                        for fn in fns:
                            fn()
                    pl.when(it == t)(run)

        slot(0)
        a[mine, mine] = dot_nt(x[cur, mine, :], x[cur, mine, :]).astype(BF16)
        slot(1)

        @pl.when(it > 0)
        def _():
            for n in (0, 1):
                x_copy(cur, n).wait_recv()
                x_copy(cur, n).wait_send()

        a_copy(0).start()
        for i in (0, 1):
            rows = ds(core * half + i * (half // 2), half // 2, 128)
            a[rows, theirs] = dot_nt(x[cur, rows, :], x[cur, theirs, :]).astype(BF16)
            a_copy(1 + i).start()
        slot(2)

        @pl.when(it < NS_STEPS - 1)
        def _():
            for n in (0, 1):
                cols = pl.ds(n * half, half)
                qacc[:, cols] = dot_nn(a[mine, mine], a[mine, cols])

        slot(3)
        for i in range(3):
            a_copy(i).wait_recv()

        @pl.when(it < NS_STEPS - 1)
        def _():
            for n in (0, 1):
                cols = pl.ds(n * half, half)
                acc = qacc[:, cols] + dot_nn(a[mine, theirs], a[theirs, cols])
                b[:, cols] = (COEF_B * a[mine, cols].astype(F32) + COEF_C * acc.astype(BF16).astype(F32)).astype(BF16)

        slot(4)
        for i in range(3):
            a_copy(i).wait_send()

        @pl.when(it < NS_STEPS - 1)
        def _():
            for n in (0, 1):
                cols = pl.ds(n * half, half)
                upd = dot_nn(b[...], x[cur, :, cols])
                x[nxt, mine, cols] = (COEF_A * x[cur, mine, cols].astype(F32) + upd.astype(BF16).astype(F32)).astype(BF16)
                x_copy(nxt, n).start()

        slot(5)
        return carry

    lax.fori_loop(0, NS_STEPS, ns_step, 0)

    def finish(k, ortho, scale):
        in_copies[k][1].wait()
        old = sc['master'][k][...]
        new = old - LEARN_RATE * (scale * ortho.astype(F32) + WEIGHT_DECAY * old)
        sc['master'][k][...] = new
        out_copy(k, 1, sc['master'][k]).start()
        sc['weight'][k][...] = new.astype(BF16)
        out_copy(k, 2, sc['weight'][k]).start()

    last = (NS_STEPS - 1) % 2
    rows_local = sc['own'][0].shape[1]
    own_rows = ds((chip * 2 + core) * rows_local, rows_local, 32)
    for n in (0, 1):
        cols = pl.ds(n * half, half)
        acc = dot_nn(a[own_rows, :], a[:, cols])
        b[0:rows_local, cols] = (COEF_B * a[own_rows, cols].astype(F32) + COEF_C * acc.astype(BF16).astype(F32)).astype(BF16)
    upd = dot_nn(b[0:rows_local, :], x[last])
    ortho = (COEF_A * x[last, own_rows, :].astype(F32) + upd.astype(BF16).astype(F32)).astype(BF16)
    finish(0, ortho, 0.2 * math.sqrt(size))

    for k in (1, 2):
        gath[k].finish()
        gath[k].drain()
    xu, tall, bu = sc['xu'], sc['tall'], sc['bu']
    small, wide = xu.shape[1], xu.shape[2]
    block = 256

    @pl.when(core == 0)
    def _():
        def flip(i, carry):
            rows = ds(i * block, block, block)
            xu[0, :, rows] = tall[rows, :].astype(F32).T.astype(BF16)
            return carry
        lax.fori_loop(0, wide // block, flip, 0)

    def ud_step(it, carry):
        cur = lax.rem(it, 2)
        nxt = 1 - cur
        gram = dot_nt(xu[cur], xu[cur]).astype(BF16)
        bu[0] = gram
        sq = dot_nn(bu[0], bu[0]).astype(BF16)
        bu[1] = (COEF_B * bu[0].astype(F32) + COEF_C * sq.astype(F32)).astype(BF16)
        for n in (0, 1):
            cols = pl.ds(n * (wide // 2), wide // 2)
            upd = dot_nn(bu[1], xu[cur, :, cols])
            xu[nxt, :, cols] = (COEF_A * xu[cur, :, cols].astype(F32) + upd.astype(BF16).astype(F32)).astype(BF16)
        return carry

    lax.fori_loop(0, NS_STEPS, ud_step, 0)
    end = NS_STEPS % 2
    up_rows, down_rows = sc['own'][1].shape[1], sc['own'][2].shape[1]
    ou, od = sc['ou'], sc['od']
    up_ref = tall.at[ds((chip * 2 + 1) * up_rows, up_rows, 32), :]
    up_copy = remote(up_ref, ou, sc['osend'].at[0], sc['orecv'].at[0], place.partner)
    down_ref = xu.at[end, ds(chip * 2 * down_rows, down_rows, 32), :]
    down_copy = remote(down_ref, od, sc['osend'].at[1], sc['orecv'].at[1], place.partner)

    @pl.when(core == 0)
    def _():
        def flip(i, carry):
            rows = ds(i * block, block, block)
            tall[rows, :] = xu[end, :, rows].astype(F32).T.astype(BF16)
            return carry
        lax.fori_loop(0, wide // block, flip, 0)
        up_copy.start()
        ou[...] = tall[ds(chip * 2 * up_rows, up_rows, 32), :]
        down_copy.wait_recv()
        up_copy.wait_send()

    @pl.when(core == 1)
    def _():
        down_copy.start()
        od[...] = xu[end, ds((chip * 2 + 1) * down_rows, down_rows, 32), :]
        up_copy.wait_recv()
        down_copy.wait_send()

    finish(1, ou[...], 0.2 * math.sqrt(wide))
    finish(2, od[...], 0.2 * math.sqrt(wide))

    for k in range(3):
        scat[k].drain()
    norm_drain(0)
    norm_drain(1)
    for k in range(3):
        out_copy(k, 0, sc['mom'][k]).wait()
        out_copy(k, 1, sc['master'][k]).wait()
        out_copy(k, 2, sc['weight'][k]).wait()


def solution(mesh):
    group = mesh.shape['data']
    chips = group // 2
    pieces = chips - 1
    grad_spec = P(('stage', 'data'), None, None, None)
    row_spec = P('stage', 'data', None)

    def step_local(*arrays):
        grads = [arrays[3 * k].reshape(arrays[3 * k].shape[2:]) for k in range(3)]
        moms = [arrays[3 * k + 1].reshape(arrays[3 * k + 1].shape[1:]) for k in range(3)]
        masters = [arrays[3 * k + 2].reshape(arrays[3 * k + 2].shape[1:]) for k in range(3)]
        shapes = [m.shape for m in moms]
        size = grads[0].shape[0]
        wide, small = grads[1].shape
        dma = pltpu.SemaphoreType.DMA
        names, scratch = [], []

        def add(name, item):
            names.append(name)
            scratch.append(item)

        for k, (rows, cols) in enumerate(shapes):
            add(('own', k), pltpu.VMEM((chips, rows, cols), F32))
            add(('pair', k), pltpu.VMEM((chips, rows, cols), F32))
            add(('ring', k), pltpu.VMEM((2, chips // 2, rows, cols), F32))
            add(('mom', k), pltpu.VMEM((rows, cols), F32))
            add(('master', k), pltpu.VMEM((rows, cols), F32))
            add(('weight', k), pltpu.VMEM((rows, cols), BF16))
        add('x', pltpu.VMEM((2, size, size), BF16))
        add('a', pltpu.VMEM((size, size), BF16))
        add('b', pltpu.VMEM((size // 2, size), BF16))
        add('qacc', pltpu.VMEM((size // 2, size), F32))
        add('tall', pltpu.VMEM((wide, small), BF16))
        add('xu', pltpu.VMEM((2, small, wide), BF16))
        add('bu', pltpu.VMEM((2, small, small), BF16))
        add('ou', pltpu.VMEM(shapes[1], BF16))
        add('od', pltpu.VMEM(shapes[2], BF16))
        add(('norm', 0), pltpu.VMEM((group, 8, 128), F32))
        add(('norm', 1), pltpu.VMEM((group, 16, 128), F32))
        for name, shape in (('load', (3, chips)), ('psend', (3, chips)), ('precv', (3, chips)), ('rsend', (3, 2, pieces)), ('rrecv', (3, 2, pieces)),
                            ('gsend', (3, 2, pieces)), ('grecv', (3, 2, pieces)), ('fsend', (3, 2, chips)), ('frecv', (3, 2, chips)),
                            ('nsend', (2, group)), ('nrecv', (2, group)), ('insem', (6,)), ('outsem', (9,)), ('asend', (3,)), ('arecv', (3,)),
                            ('xsend', (2,)), ('xrecv', (2,)), ('osend', (2,)), ('orecv', (2,))):
            add(name, dma(shape))

        def body(*refs):
            sc = {}
            for name, ref in zip(names, refs[18:]):
                if isinstance(name, tuple):
                    sc.setdefault(name[0], []).append(ref)
                else:
                    sc[name] = ref
            kernel(group, refs[0:3], refs[3:6], refs[6:9], refs[9:18], sc)

        out_shape = []
        for shape in shapes:
            out_shape += [jax.ShapeDtypeStruct(shape, F32), jax.ShapeDtypeStruct(shape, F32), jax.ShapeDtypeStruct(shape, BF16)]
        results = pl.pallas_call(
            body,
            out_shape=tuple(out_shape),
            in_specs=[pl.BlockSpec(memory_space=pl.ANY)] * 9,
            out_specs=tuple([pl.BlockSpec(memory_space=pl.ANY)] * 9),
            scratch_shapes=scratch,
            compiler_params=pltpu.CompilerParams(collective_id=0, has_side_effects=True, vmem_limit_bytes=64 * 1024 * 1024 - 65536),
            name='muon',
        )(*grads, *moms, *masters)
        return tuple(r[None] for r in results)

    in_specs = (grad_spec, row_spec, row_spec) * 3
    out_specs = (row_spec,) * 9
    return jax.shard_map(step_local, mesh=mesh, in_specs=in_specs, out_specs=out_specs, check_vma=False)
```

```python
import functools
import math
import jax
import jax.numpy as jnp
from jax import lax
from jax.experimental import pallas as pl
from jax.experimental.pallas import tpu as pltpu
from jax.sharding import PartitionSpec as P

MOMENTUM = 0.95
LEARN_RATE = 0.25
WEIGHT_DECAY = 0.2
EPSILON = 1e-7
COEF_A = 3.4445
COEF_B = -4.7750
COEF_C = 2.0315
NS_STEPS = 5
F32 = jnp.float32
BF16 = jnp.bfloat16


def dot_nn(a, b):
    return lax.dot_general(a, b, (((1,), (0,)), ((), ())), preferred_element_type=F32)


def dot_tn(a, b):
    return lax.dot_general(a, b, (((0,), (0,)), ((), ())), preferred_element_type=F32)


def dot_nt(a, b):
    return lax.dot_general(a, b, (((1,), (1,)), ((), ())), preferred_element_type=F32)


def remote(src, dst, send_sem, recv_sem, dev):
    return pltpu.make_async_remote_copy(
        src_ref=src, dst_ref=dst, send_sem=send_sem, recv_sem=recv_sem,
        device_id={'data': dev}, device_id_type=pl.DeviceIdType.MESH)


def ds(start, size, mult):
    return pl.ds(pl.multiple_of(start, mult), size)


class Place:
    def __init__(self, group):
        self.group = group
        self.chips = group // 2
        self.me = lax.axis_index('data')
        self.chip = self.me // 2
        self.core = self.me % 2
        self.partner = self.chip * 2 + (1 - self.core)

    def at(self, offset):
        return lax.rem(self.chip + offset + self.chips, self.chips)

    def next(self, way):
        return self.at(1 if way == 0 else -1) * 2 + self.core


class Scatter:
    def __init__(self, place, grad, own, pair, ring, load, psend, precv, rsend, rrecv):
        self.pl, self.grad, self.own, self.pair, self.ring = place, grad, own, pair, ring
        self.load, self.psend, self.precv, self.rsend, self.rrecv = load, psend, precv, rsend, rrecv
        self.rows = own.shape[1]
        self.half_rows = self.rows // 2
        self.n = place.chips
        self.pieces = self.n - 1

    def order(self):
        far = self.n // 2
        order = [far]
        for d in range(far - 1, 0, -1):
            order += [d, self.n - d]
        return order + [0]

    def load_copy(self, d):
        row = (self.pl.at(d) * 2 + self.pl.core) * self.rows
        return pltpu.make_async_copy(self.grad.at[ds(row, self.rows, 32), :], self.own.at[d], self.load.at[d])

    def pair_copy(self, d):
        row = (self.pl.at(d) * 2 + (1 - self.pl.core)) * self.rows
        return remote(self.grad.at[ds(row, self.rows, 32), :], self.pair.at[d], self.psend.at[d], self.precv.at[d], self.pl.partner)

    def start(self):
        for d in self.order():
            self.pair_copy(d).start()
            self.load_copy(d).start()

    def arrive(self, d):
        self.load_copy(d).wait()
        self.pair_copy(d).wait_recv()

    def spot(self, way, q):
        dist = self.n // 2 - (q + 1) // 2
        half = way if q % 2 == 0 else 1 - way
        return dist, (dist if way == 0 else (self.n - dist) % self.n), pl.ds(half * self.half_rows, self.half_rows)

    def ring_copy(self, way, q):
        dist, d, rows = self.spot(way, q)
        return remote(self.own.at[d, rows, :], self.ring.at[way, dist - 1, rows, :], self.rsend.at[way, q], self.rrecv.at[way, q], self.pl.next(way))

    def step(self, q):
        for way in (0, 1):
            dist, d, rows = self.spot(way, q)
            if q % 2 == 1 or (q == 0 and way == 0):
                self.arrive(d)
            total = self.own[d, rows, :] + self.pair[d, rows, :]
            if q >= 2:
                self.ring_copy(way, q - 2).wait_recv()
                total = total + self.ring[way, dist, rows, :]
            self.own[d, rows, :] = total
            self.ring_copy(way, q).start()

    def total(self):
        self.arrive(0)
        for way in (0, 1):
            for q in (self.pieces - 2, self.pieces - 1):
                self.ring_copy(way, q).wait_recv()
        return (self.own[0] + self.pair[0]) + (self.ring[0, 0] + self.ring[1, 0])

    def drain(self):
        for d in range(self.n):
            self.pair_copy(d).wait_send()
        for way in (0, 1):
            for q in range(self.pieces):
                self.ring_copy(way, q).wait_send()


class Gather:
    def __init__(self, place, full, rows, panels, rsend, rrecv, fsend, frecv):
        self.pl, self.full, self.rows, self.panels = place, full, rows, panels
        self.rsend, self.rrecv, self.fsend, self.frecv = rsend, rrecv, fsend, frecv
        self.half_rows = rows // 2
        self.n = place.chips
        self.pieces = self.n - 1

    def base(self, chip, core):
        return ((core * self.n + chip) if self.panels else (chip * 2 + core)) * self.rows

    def piece(self, way, q, core, lag):
        hop = q // 2 + lag
        chip = self.pl.at(-hop if way == 0 else hop)
        half = way if q % 2 == 0 else 1 - way
        row = self.base(chip, core) + half * self.half_rows
        return self.full.at[ds(row, self.half_rows, 16), :]

    def ring_copy(self, way, q):
        ref = self.piece(way, q, self.pl.core, 0)
        return remote(ref, ref, self.rsend.at[way, q], self.rrecv.at[way, q], self.pl.next(way))

    def arrival(self, way, q):
        ref = self.piece(way, q, self.pl.core, 1)
        return remote(ref, ref, self.rsend.at[way, q], self.rrecv.at[way, q], self.pl.next(way))

    def forward(self, way, q, core):
        ref = self.piece(way, q, core, 1)
        return remote(ref, ref, self.fsend.at[way, q], self.frecv.at[way, q], self.pl.partner)

    def own_rows(self, core):
        return self.full.at[ds(self.base(self.pl.chip, core), self.rows, 32), :]

    def forward_own(self, core):
        ref = self.own_rows(core)
        return remote(ref, ref, self.fsend.at[0, self.pieces], self.frecv.at[0, self.pieces], self.pl.partner)

    def step(self, q):
        if q == 0:
            for k in (0, 1):
                for way in (0, 1):
                    self.ring_copy(way, k).start()
            self.forward_own(self.pl.core).start()
        else:
            for way in (0, 1):
                self.arrival(way, q - 1).wait_recv()
                if q + 1 < self.pieces:
                    self.ring_copy(way, q + 1).start()
                self.forward(way, q - 1, self.pl.core).start()

    def steps(self):
        return self.pieces + 1

    def finish(self):
        self.forward_own(1 - self.pl.core).wait_recv()
        for way in (0, 1):
            for q in range(self.pieces):
                self.forward(way, q, 1 - self.pl.core).wait_recv()

    def drain(self):
        self.forward_own(self.pl.core).wait_send()
        for way in (0, 1):
            for q in range(self.pieces):
                self.forward(way, q, self.pl.core).wait_send()
                self.ring_copy(way, q).wait_send()


def squares(mat):
    sq = mat * mat
    rows, cols = mat.shape
    acc = sq[0:8]
    for i in range(1, rows // 8):
        acc = acc + sq[8 * i:8 * i + 8]
    out = acc[:, 0:128]
    for j in range(1, cols // 128):
        out = out + acc[:, 128 * j:128 * j + 128]
    return out


def total_norm(ref, top):
    acc = ref[0, top:top + 8]
    for i in range(1, ref.shape[0]):
        acc = acc + ref[i, top:top + 8]
    total = jnp.sum(jnp.sum(acc, axis=1, keepdims=True), axis=0, keepdims=True)
    return jnp.sqrt(total) + EPSILON


def kernel(group, grads, moms, outs, sc):
    place = Place(group)
    core, chip = place.core, place.chip
    chips = place.chips
    pieces = chips - 1
    barrier = pltpu.get_barrier_semaphore()
    for dev in (place.partner, place.next(0), place.next(1)):
        pl.semaphore_signal(barrier, inc=1, device_id={'data': dev}, device_id_type=pl.DeviceIdType.MESH)
    pl.semaphore_wait(barrier, 3)

    scat = [Scatter(place, grads[k], sc['own'][k], sc['pair'][k], sc['ring'][k], sc['load'].at[k], sc['psend'].at[k], sc['precv'].at[k],
                    sc['rsend'].at[k], sc['rrecv'].at[k]) for k in range(3)]
    fulls = [sc['x'][0], sc['tall'], sc['xd']]
    gath = [Gather(place, fulls[k], sc['own'][k].shape[1], k == 0, sc['gsend'].at[k], sc['grecv'].at[k], sc['fsend'].at[k], sc['frecv'].at[k]) for k in range(3)]

    scat[0].start()
    in_copies = []
    for k in range(3):
        in_copies.append(pltpu.make_async_copy(moms[k], sc['mom'][k], sc['insem'].at[k]))
        in_copies[k].start()
    scat[1].start()
    scat[2].start()

    def out_copy(k, j, ref):
        return pltpu.make_async_copy(ref, outs[2 * k + j], sc['outsem'].at[2 * k + j])

    def momentum(k):
        in_copies[k].wait()
        mat = MOMENTUM * sc['mom'][k][...] + scat[k].total() * (1.0 / group)
        sc['mom'][k][...] = mat
        out_copy(k, 0, sc['mom'][k]).start()
        return squares(mat)

    def norm_copy(idx, i):
        ref = sc['norm'][idx]
        dev = lax.rem(place.me + i, group)
        return remote(ref.at[0], ref.at[i], sc['nsend'].at[idx, i], sc['nrecv'].at[idx, i], dev)

    def norm_send(idx):
        for i in range(1, group):
            norm_copy(idx, i).start()

    def norm_wait(idx):
        for i in range(1, group):
            norm_copy(idx, i).wait_recv()

    def norm_drain(idx):
        for i in range(1, group):
            norm_copy(idx, i).wait_send()

    def write_x(k, norm):
        rows = sc['own'][k].shape[1]
        fulls[k][ds(gath[k].base(chip, core), rows, 32), :] = (sc['mom'][k][...] / norm).astype(BF16)

    for q in range(pieces):
        scat[0].step(q)
    sc['norm'][0][0] = momentum(0)
    norm_send(0)
    for q in (0, 1):
        for k in (1, 2):
            scat[k].step(q)
    norm_wait(0)
    write_x(0, total_norm(sc['norm'][0], 0))
    for q in range(gath[0].steps()):
        gath[0].step(q)
        if q + 2 == pieces:
            for k in (1, 2):
                scat[k].step(2)

    tasks = {}

    def background(it, slot, fn):
        tasks.setdefault((it, slot), []).append(fn)

    def ud_momentum():
        sc['norm'][1][0, 0:8] = momentum(1)
        sc['norm'][1][0, 8:16] = momentum(2)
        norm_send(1)

    def ud_write():
        norm_wait(1)
        write_x(1, total_norm(sc['norm'][1], 0))
        write_x(2, total_norm(sc['norm'][1], 8))

    def both(parts, q):
        def run():
            parts[1].step(q)
            parts[2].step(q)
        return run

    background(0, 0, both(scat, 3))
    for q, place_at in ((4, (0, 3)), (5, (0, 5)), (6, (1, 1))):
        background(*place_at, both(scat, q))
    background(1, 5, ud_momentum)
    background(2, 2, ud_write)
    times = ((2, 2), (2, 5), (2, 6), (3, 1), (3, 2), (3, 3), (3, 5), (3, 6))
    for q in range(gath[1].steps()):
        background(*times[q], both(gath, q))

    xs, a, b, qacc = sc['x'], sc['a'], sc['b'], sc['qacc']
    size = a.shape[0]
    half = size // 2
    third = size // 3
    mine = ds(core * half, half, 128)
    theirs = ds((1 - core) * half, half, 128)

    def a_copy(i):
        if i == 0:
            return remote(a.at[mine, mine], a.at[mine, mine], sc['asend'].at[0], sc['arecv'].at[0], place.partner)
        rows = ds(core * half + (i - 1) * (half // 2), half // 2, 128)
        return remote(a.at[rows, theirs], a.at[rows, theirs], sc['asend'].at[i], sc['arecv'].at[i], place.partner)

    def x_copy(x, n):
        ref = x.at[mine, pl.ds(n * third, third)]
        return remote(ref, ref, sc['xsend'].at[n], sc['xrecv'].at[n], place.partner)

    def x_wait(x):
        for n in range(3):
            x_copy(x, n).wait_recv()
            x_copy(x, n).wait_send()

    def grams(x, slot, wait):
        slot(0)
        a[mine, mine] = dot_nt(x[mine, :], x[mine, :]).astype(BF16)
        wait()
        slot(1)
        a_copy(0).start()
        for i in (0, 1):
            rows = ds(core * half + i * (half // 2), half // 2, 128)
            a[rows, theirs] = dot_nt(x[rows, :], x[theirs, :]).astype(BF16)
            a_copy(1 + i).start()

    def a_wait():
        for i in range(3):
            a_copy(i).wait_recv()

    def a_drain():
        for i in range(3):
            a_copy(i).wait_send()

    def poly(lin, acc):
        return (COEF_B * lin.astype(F32) + COEF_C * acc.astype(BF16).astype(F32)).astype(BF16)

    def renew(old, upd):
        return (COEF_A * old.astype(F32) + upd.astype(BF16).astype(F32)).astype(BF16)

    def ns_step(pair, parity):
        x, xn = xs[parity], xs[1 - parity]

        def slot(s):
            for (t, u), fns in tasks.items():
                if u == s and t % 2 == parity:
                    def run(fns=fns):
                        for fn in fns:
                            fn()
                    pl.when(pair == t // 2)(run)

        def wait():
            if parity == 0:
                @pl.when(pair == 0)
                def _():
                    gath[0].finish()
                    gath[0].drain()

                @pl.when(pair > 0)
                def _():
                    x_wait(x)
            else:
                x_wait(x)

        grams(x, slot, wait)
        slot(2)
        for n in (0, 1):
            cols = pl.ds(n * half, half)
            qacc[:, cols] = dot_nn(a[mine, mine], a[mine, cols])
        slot(3)
        a_wait()
        for n in (0, 1):
            cols = pl.ds(n * half, half)
            b[:, cols] = poly(a[mine, cols], qacc[:, cols] + dot_nn(a[mine, theirs], a[theirs, cols]))
        slot(4)
        a_drain()
        for n in range(3):
            cols = pl.ds(n * third, third)
            xn[mine, cols] = renew(x[mine, cols], dot_nn(b[...], x[:, cols]))
            x_copy(xn, n).start()
            if n < 2:
                slot(5 + n)

    def ns_pair(pair, carry):
        ns_step(pair, 0)
        ns_step(pair, 1)
        return carry

    lax.fori_loop(0, NS_STEPS // 2, ns_pair, 0)

    x = xs[0]
    grams(x, lambda s: None, lambda: x_wait(x))
    a_wait()
    rows_local = sc['own'][0].shape[1]
    own_rows = ds(core * half + chip * rows_local, rows_local, 32)
    for n in (0, 1):
        cols = pl.ds(n * half, half)
        b[0:rows_local, cols] = poly(a[own_rows, cols], dot_nn(a[own_rows, :], a[:, cols]))
    a_drain()
    sc['oa'][...] = renew(x[own_rows, :], dot_nn(b[0:rows_local, :], x[...]))
    out_copy(0, 1, sc['oa']).start()

    for k in (1, 2):
        gath[k].finish()
        gath[k].drain()
    xd, tall, bu = sc['xd'], sc['tall'], sc['bu']
    small, wide = xd.shape
    up_rows, down_rows = sc['own'][1].shape[1], sc['own'][2].shape[1]
    up_send, down_send = sc['up_send'], sc['down_send']
    up_copy = remote(up_send, sc['ou'], sc['osend'].at[0], sc['orecv'].at[0], place.partner)
    down_copy = remote(down_send, sc['od'], sc['osend'].at[1], sc['orecv'].at[1], place.partner)
    half_wide = wide // 2

    @pl.when(core == 0)
    def _():
        def step(it, carry):
            bu[0] = dot_tn(tall[...], tall[...]).astype(BF16)
            bu[1] = poly(bu[0], dot_nn(bu[0], bu[0]))
            for n in (0, 1):
                rows = pl.ds(n * half_wide, half_wide)
                tall[rows, :] = renew(tall[rows, :], dot_nn(tall[rows, :], bu[1]))
            return carry
        lax.fori_loop(0, NS_STEPS - 1, step, 0)
        bu[0] = dot_tn(tall[...], tall[...]).astype(BF16)
        bu[1] = poly(bu[0], dot_nn(bu[0], bu[0]))
        other = tall[ds((chip * 2 + 1) * up_rows, up_rows, 32), :]
        up_send[...] = renew(other, dot_nn(other, bu[1]))
        up_copy.start()
        own = tall[ds(chip * 2 * up_rows, up_rows, 32), :]
        sc['ou'][...] = renew(own, dot_nn(own, bu[1]))
        out_copy(1, 1, sc['ou']).start()
        down_copy.wait_recv()
        out_copy(2, 1, sc['od']).start()
        up_copy.wait_send()

    @pl.when(core == 1)
    def _():
        def step(it, carry):
            bu[0] = dot_nt(xd[...], xd[...]).astype(BF16)
            bu[1] = poly(bu[0], dot_nn(bu[0], bu[0]))
            for n in (0, 1):
                cols = pl.ds(n * half_wide, half_wide)
                xd[:, cols] = renew(xd[:, cols], dot_nn(bu[1], xd[:, cols]))
            return carry
        lax.fori_loop(0, NS_STEPS - 1, step, 0)
        bu[0] = dot_nt(xd[...], xd[...]).astype(BF16)

        def rows_of(which):
            rows = ds((chip * 2 + which) * down_rows, down_rows, 32)
            part = poly(bu[0, rows, :], dot_nn(bu[0, rows, :], bu[0]))
            return renew(xd[rows, :], dot_nn(part, xd[...]))
        down_send[...] = rows_of(0)
        down_copy.start()
        sc['od'][...] = rows_of(1)
        out_copy(2, 1, sc['od']).start()
        up_copy.wait_recv()
        out_copy(1, 1, sc['ou']).start()
        down_copy.wait_send()

    for k in range(3):
        scat[k].drain()
    norm_drain(0)
    norm_drain(1)
    for k in range(3):
        out_copy(k, 0, sc['mom'][k]).wait()
        out_copy(k, 1, sc[('oa', 'ou', 'od')[k]]).wait()


def results_kernel(scales, *refs):
    for k in range(3):
        mom, ortho, master = refs[k], refs[3 + k], refs[6 + k]
        mom_out, master_out, weight_out = refs[9 + 3 * k:12 + 3 * k]
        mom_out[...] = mom[...]
        old = master[...]
        new = old - LEARN_RATE * (scales[k] * ortho[...].astype(F32) + WEIGHT_DECAY * old)
        master_out[...] = new
        weight_out[...] = new.astype(BF16)


def solution(mesh):
    group = mesh.shape['data']
    chips = group // 2
    pieces = chips - 1
    grad_spec = P(('stage', 'data'), None, None, None)
    row_spec = P('stage', 'data', None)

    def step_local(*arrays):
        grads = [arrays[3 * k].reshape(arrays[3 * k].shape[2:]) for k in range(3)]
        moms = [arrays[3 * k + 1].reshape(arrays[3 * k + 1].shape[1:]) for k in range(3)]
        masters = [arrays[3 * k + 2].reshape(arrays[3 * k + 2].shape[1:]) for k in range(3)]
        shapes = [m.shape for m in moms]
        size = grads[0].shape[0]
        wide, small = grads[1].shape
        dma = pltpu.SemaphoreType.DMA
        names, scratch = [], []

        def add(name, item):
            names.append(name)
            scratch.append(item)

        for k, (rows, cols) in enumerate(shapes):
            add(('own', k), pltpu.VMEM((chips, rows, cols), F32))
            add(('pair', k), pltpu.VMEM((chips, rows, cols), F32))
            add(('ring', k), pltpu.VMEM((2, chips // 2, rows, cols), F32))
            add(('mom', k), pltpu.VMEM((rows, cols), F32))
        add(('x', 0), pltpu.VMEM((size, size), BF16))
        add(('x', 1), pltpu.VMEM((size, size), BF16))
        add('a', pltpu.VMEM((size, size), BF16))
        add('b', pltpu.VMEM((size // 2, size), BF16))
        add('qacc', pltpu.VMEM((size // 2, size), F32))
        add('tall', pltpu.VMEM((wide, small), BF16))
        add('xd', pltpu.VMEM((small, wide), BF16))
        add('bu', pltpu.VMEM((2, small, small), BF16))
        for name, k in (('oa', 0), ('ou', 1), ('od', 2), ('up_send', 1), ('down_send', 2)):
            add(name, pltpu.VMEM(shapes[k], BF16))
        add(('norm', 0), pltpu.VMEM((group, 8, 128), F32))
        add(('norm', 1), pltpu.VMEM((group, 16, 128), F32))
        for name, shape in (('load', (3, chips)), ('psend', (3, chips)), ('precv', (3, chips)), ('rsend', (3, 2, pieces)), ('rrecv', (3, 2, pieces)),
                            ('gsend', (3, 2, pieces)), ('grecv', (3, 2, pieces)), ('fsend', (3, 2, chips)), ('frecv', (3, 2, chips)),
                            ('nsend', (2, group)), ('nrecv', (2, group)), ('insem', (3,)), ('outsem', (6,)), ('asend', (3,)), ('arecv', (3,)),
                            ('xsend', (3,)), ('xrecv', (3,)), ('osend', (2,)), ('orecv', (2,))):
            add(name, dma(shape))

        def body(*refs):
            sc = {}
            for name, ref in zip(names, refs[12:]):
                if isinstance(name, tuple):
                    sc.setdefault(name[0], []).append(ref)
                else:
                    sc[name] = ref
            kernel(group, refs[0:3], refs[3:6], refs[6:12], sc)

        anywhere = pl.BlockSpec(memory_space=pl.ANY)
        part_shape = []
        for shape in shapes:
            part_shape += [jax.ShapeDtypeStruct(shape, F32), jax.ShapeDtypeStruct(shape, BF16)]
        parts = pl.pallas_call(
            body,
            out_shape=tuple(part_shape),
            in_specs=[anywhere] * 6,
            out_specs=tuple([anywhere] * 6),
            scratch_shapes=scratch,
            compiler_params=pltpu.CompilerParams(collective_id=0, has_side_effects=True, vmem_limit_bytes=64 * 1024 * 1024 - 65536),
            name='muon',
        )(*grads, *moms)
        scales = [0.2 * math.sqrt(max(g.shape)) for g in grads]
        out_shape = []
        for shape in shapes:
            out_shape += [jax.ShapeDtypeStruct(shape, F32), jax.ShapeDtypeStruct(shape, F32), jax.ShapeDtypeStruct(shape, BF16)]
        vmem = pl.BlockSpec(memory_space=pltpu.VMEM)
        results = pl.pallas_call(
            functools.partial(results_kernel, scales),
            out_shape=tuple(out_shape),
            in_specs=[vmem] * 9,
            out_specs=tuple([vmem] * 9),
            name='results',
        )(*parts[0::2], *parts[1::2], *masters)
        return tuple(r[None] for r in results)

    in_specs = (grad_spec, row_spec, row_spec) * 3
    out_specs = (row_spec,) * 9
    return jax.shard_map(step_local, mesh=mesh, in_specs=in_specs, out_specs=out_specs, check_vma=False)
```

```python
import functools
import math
import jax
import jax.numpy as jnp
from jax import lax
from jax.experimental import pallas as pl
from jax.experimental.pallas import tpu as pltpu
from jax.sharding import PartitionSpec as P

MOMENTUM = 0.95
LEARN_RATE = 0.25
WEIGHT_DECAY = 0.2
EPSILON = 1e-7
COEF_A = 3.4445
COEF_B = -4.7750
COEF_C = 2.0315
NS_STEPS = 5
F32 = jnp.float32
BF16 = jnp.bfloat16


def dot_nn(a, b):
    return lax.dot_general(a, b, (((1,), (0,)), ((), ())), preferred_element_type=F32)


def dot_tn(a, b):
    return lax.dot_general(a, b, (((0,), (0,)), ((), ())), preferred_element_type=F32)


def dot_nt(a, b):
    return lax.dot_general(a, b, (((1,), (1,)), ((), ())), preferred_element_type=F32)


def remote(src, dst, send_sem, recv_sem, dev):
    return pltpu.make_async_remote_copy(
        src_ref=src, dst_ref=dst, send_sem=send_sem, recv_sem=recv_sem,
        device_id={'data': dev}, device_id_type=pl.DeviceIdType.MESH)


def ds(start, size, mult):
    return pl.ds(pl.multiple_of(start, mult), size)


class Place:
    def __init__(self, group):
        self.group = group
        self.chips = group // 2
        self.me = lax.axis_index('data')
        self.chip = self.me // 2
        self.core = self.me % 2
        self.partner = self.chip * 2 + (1 - self.core)

    def at(self, offset):
        return lax.rem(self.chip + offset + self.chips, self.chips)

    def next(self, way):
        return self.at(1 if way == 0 else -1) * 2 + self.core


class Scatter:
    def __init__(self, place, grad, own, pair, ring, load, psend, precv, rsend, rrecv):
        self.pl, self.grad, self.own, self.pair, self.ring = place, grad, own, pair, ring
        self.load, self.psend, self.precv, self.rsend, self.rrecv = load, psend, precv, rsend, rrecv
        self.rows = own.shape[1]
        self.half_rows = self.rows // 2
        self.n = place.chips
        self.pieces = self.n - 1

    def order(self):
        far = self.n // 2
        order = [far]
        for d in range(far - 1, 0, -1):
            order += [d, self.n - d]
        return order + [0]

    def load_copy(self, d):
        row = (self.pl.at(d) * 2 + self.pl.core) * self.rows
        return pltpu.make_async_copy(self.grad.at[ds(row, self.rows, 32), :], self.own.at[d], self.load.at[d])

    def pair_copy(self, d):
        row = (self.pl.at(d) * 2 + (1 - self.pl.core)) * self.rows
        return remote(self.grad.at[ds(row, self.rows, 32), :], self.pair.at[d], self.psend.at[d], self.precv.at[d], self.pl.partner)

    def start(self):
        for d in self.order():
            self.pair_copy(d).start()
            self.load_copy(d).start()

    def arrive(self, d):
        self.load_copy(d).wait()
        self.pair_copy(d).wait_recv()

    def spot(self, way, q):
        dist = self.n // 2 - (q + 1) // 2
        half = way if q % 2 == 0 else 1 - way
        return dist, (dist if way == 0 else (self.n - dist) % self.n), pl.ds(half * self.half_rows, self.half_rows)

    def ring_copy(self, way, q):
        dist, d, rows = self.spot(way, q)
        return remote(self.own.at[d, rows, :], self.ring.at[way, dist - 1, rows, :], self.rsend.at[way, q], self.rrecv.at[way, q], self.pl.next(way))

    def step(self, q):
        for way in (0, 1):
            dist, d, rows = self.spot(way, q)
            if q % 2 == 1 or (q == 0 and way == 0):
                self.arrive(d)
            total = self.own[d, rows, :] + self.pair[d, rows, :]
            if q >= 2:
                self.ring_copy(way, q - 2).wait_recv()
                total = total + self.ring[way, dist, rows, :]
            self.own[d, rows, :] = total
            self.ring_copy(way, q).start()

    def total(self):
        self.arrive(0)
        for way in (0, 1):
            for q in (self.pieces - 2, self.pieces - 1):
                self.ring_copy(way, q).wait_recv()
        return (self.own[0] + self.pair[0]) + (self.ring[0, 0] + self.ring[1, 0])

    def drain(self):
        for d in range(self.n):
            self.pair_copy(d).wait_send()
        for way in (0, 1):
            for q in range(self.pieces):
                self.ring_copy(way, q).wait_send()


class Gather:
    def __init__(self, place, full, other, rows, to, rsend, rrecv, fsend, frecv):
        self.pl, self.full, self.other, self.rows, self.to = place, full, other, rows, to
        self.rsend, self.rrecv, self.fsend, self.frecv = rsend, rrecv, fsend, frecv
        self.half_rows = rows // 2
        self.n = place.chips
        self.pieces = self.n - 1

    def rows_of(self, way, q, lag):
        hop = q // 2 + lag
        slot = 0 if hop == 0 else min(2 * hop - 1 + way, self.n - 1)
        half = way if q % 2 == 0 else 1 - way
        return pl.ds(slot * self.rows + half * self.half_rows, self.half_rows)

    def ring_copy(self, way, q):
        return remote(self.full.at[self.rows_of(way, q, 0), :], self.full.at[self.rows_of(way, q, 1), :],
                      self.rsend.at[way, q], self.rrecv.at[way, q], self.pl.next(way))

    def forward(self, way, q):
        rows = self.rows_of(way, q, 1)
        return remote(self.full.at[rows, :], self.other.at[rows, :], self.fsend.at[way, q], self.frecv.at[way, q], self.pl.partner)

    def forward_own(self):
        rows = pl.ds(0, self.rows)
        return remote(self.full.at[rows, :], self.other.at[rows, :], self.fsend.at[0, self.pieces], self.frecv.at[0, self.pieces], self.pl.partner)

    def sending(self, fn):
        if self.to is None:
            fn()
        else:
            pl.when(self.pl.core != self.to)(fn)

    def step(self, q):
        if q == 0:
            for k in (0, 1):
                for way in (0, 1):
                    self.ring_copy(way, k).start()
            self.sending(lambda: self.forward_own().start())
        else:
            for way in (0, 1):
                self.ring_copy(way, q - 1).wait_recv()
                if q + 1 < self.pieces:
                    self.ring_copy(way, q + 1).start()

            def hand_on():
                for way in (0, 1):
                    self.forward(way, q - 1).start()
            self.sending(hand_on)

    def steps(self):
        return self.pieces + 1

    def finish(self):
        def run():
            self.forward_own().wait_recv()
            for way in (0, 1):
                for q in range(self.pieces):
                    self.forward(way, q).wait_recv()
        if self.to is None:
            run()
        else:
            pl.when(self.pl.core == self.to)(run)

    def drain(self):
        for way in (0, 1):
            for q in range(self.pieces):
                self.ring_copy(way, q).wait_send()

        def run():
            self.forward_own().wait_send()
            for way in (0, 1):
                for q in range(self.pieces):
                    self.forward(way, q).wait_send()
        self.sending(run)


def squares(mat):
    sq = mat * mat
    rows, cols = mat.shape
    acc = sq[0:8]
    for i in range(1, rows // 8):
        acc = acc + sq[8 * i:8 * i + 8]
    out = acc[:, 0:128]
    for j in range(1, cols // 128):
        out = out + acc[:, 128 * j:128 * j + 128]
    return out


def total_norm(ref, top):
    acc = ref[0, top:top + 8]
    for i in range(1, ref.shape[0]):
        acc = acc + ref[i, top:top + 8]
    total = jnp.sum(jnp.sum(acc, axis=1, keepdims=True), axis=0, keepdims=True)
    return jnp.sqrt(total) + EPSILON


def kernel(group, grads, moms, outs, sc):
    place = Place(group)
    core, chip = place.core, place.chip
    chips = place.chips
    pieces = chips - 1
    barrier = pltpu.get_barrier_semaphore()
    for dev in (place.partner, place.next(0), place.next(1)):
        pl.semaphore_signal(barrier, inc=1, device_id={'data': dev}, device_id_type=pl.DeviceIdType.MESH)
    pl.semaphore_wait(barrier, 3)

    scat = [Scatter(place, grads[k], sc['own'][k], sc['pair'][k], sc['ring'][k], sc['load'].at[k], sc['psend'].at[k], sc['precv'].at[k],
                    sc['rsend'].at[k], sc['rrecv'].at[k]) for k in range(3)]
    xo, xp = sc['xo'], sc['xp']
    xd, tall = sc['xd'], sc['tall']
    small, wide = xd.shape
    fulls = [xo[0], tall.at[pl.ds(0, wide // 2), :], xd.at[pl.ds(0, small // 2), :]]
    others = [xp[0], tall.at[pl.ds(wide // 2, wide // 2), :], xd.at[pl.ds(small // 2, small // 2), :]]
    gath = [Gather(place, fulls[k], others[k], sc['own'][k].shape[1], (None, 0, 1)[k], sc['gsend'].at[k], sc['grecv'].at[k], sc['fsend'].at[k], sc['frecv'].at[k])
            for k in range(3)]

    scat[0].start()
    in_copies = []
    for k in range(3):
        in_copies.append(pltpu.make_async_copy(moms[k], sc['mom'][k], sc['insem'].at[k]))
        in_copies[k].start()
    scat[1].start()
    scat[2].start()

    def out_copy(k, j, ref):
        return pltpu.make_async_copy(ref, outs[2 * k + j], sc['outsem'].at[2 * k + j])

    def momentum(k):
        in_copies[k].wait()
        mat = MOMENTUM * sc['mom'][k][...] + scat[k].total() * (1.0 / group)
        sc['mom'][k][...] = mat
        out_copy(k, 0, sc['mom'][k]).start()
        return squares(mat)

    def norm_copy(idx, i):
        ref = sc['norm'][idx]
        dev = lax.rem(place.me + i, group)
        return remote(ref.at[0], ref.at[i], sc['nsend'].at[idx, i], sc['nrecv'].at[idx, i], dev)

    def norm_send(idx):
        for i in range(1, group):
            norm_copy(idx, i).start()

    def norm_wait(idx):
        for i in range(1, group):
            norm_copy(idx, i).wait_recv()

    def norm_drain(idx):
        for i in range(1, group):
            norm_copy(idx, i).wait_send()

    def write_x(k, norm):
        rows = sc['own'][k].shape[1]
        fulls[k][0:rows, :] = (sc['mom'][k][...] / norm).astype(BF16)

    for q in range(pieces):
        scat[0].step(q)
    sc['norm'][0][0] = momentum(0)
    norm_send(0)
    for q in (0, 1):
        for k in (1, 2):
            scat[k].step(q)
    norm_wait(0)
    write_x(0, total_norm(sc['norm'][0], 0))
    for q in range(gath[0].steps()):
        gath[0].step(q)
        if q + 2 == pieces:
            for k in (1, 2):
                scat[k].step(2)

    tasks = {}

    def background(it, slot, fn):
        tasks.setdefault((it, slot), []).append(fn)

    def ud_momentum():
        sc['norm'][1][0, 0:8] = momentum(1)
        sc['norm'][1][0, 8:16] = momentum(2)
        norm_send(1)

    def ud_write():
        norm_wait(1)
        write_x(1, total_norm(sc['norm'][1], 0))
        write_x(2, total_norm(sc['norm'][1], 8))

    def both(parts, q):
        def run():
            parts[1].step(q)
            parts[2].step(q)
        return run

    background(0, 0, both(scat, 3))
    for q, place_at in ((4, (0, 4)), (5, (0, 7)), (6, (1, 2))):
        background(*place_at, both(scat, q))
    background(1, 7, ud_momentum)
    background(2, 4, ud_write)
    times = ((2, 4), (2, 7), (3, 1), (3, 3), (3, 5), (3, 6), (4, 0), (4, 2))
    for q in range(gath[1].steps()):
        background(*times[q], both(gath, q))

    aoo, aop, app, ar = sc['aoo'], sc['aop'], sc['app'], sc['ar']
    bo, bp = sc['bo'], sc['bp']
    half, size = xo[0].shape
    third = size // 3
    parts = 3
    blk = half // parts

    def rows_at(i):
        return pl.ds(i * blk, blk)

    def cross_copy(t):
        return remote(aop.at[rows_at(t), rows_at((t + 1) % parts)], ar.at[t], sc['asend'].at[t], sc['arecv'].at[t], place.partner)

    def own_copy():
        return remote(aoo, app, sc['asend'].at[parts], sc['arecv'].at[parts], place.partner)

    def x_copy(way, n):
        cols = pl.ds(n * third, third)
        return remote(xo[way].at[:, cols], xp[way].at[:, cols], sc['xsend'].at[n], sc['xrecv'].at[n], place.partner)

    def x_wait(way):
        for n in range(3):
            x_copy(way, n).wait_recv()
            x_copy(way, n).wait_send()

    def mirror(ref):
        for i in range(parts):
            for j in range(i + 1, parts):
                ref[rows_at(j), rows_at(i)] = ref[rows_at(i), rows_at(j)].T

    def grams(way, slot, wait):
        x, y = xo[way], xp[way]
        slot(0)
        for i in range(parts):
            aoo[rows_at(i), i * blk:] = dot_nt(x[rows_at(i), :], x[i * blk:, :]).astype(BF16)
        slot(1)
        wait()
        for t in range(parts):
            u = (t + 1) % parts
            aop[rows_at(t), rows_at(u)] = dot_nt(x[rows_at(t), :], y[rows_at(u), :]).astype(BF16)
        for t in range(parts):
            cross_copy(t).start()
        slot(2)
        for t in range(parts):
            aop[rows_at(t), rows_at(t)] = dot_nt(x[rows_at(t), :], y[rows_at(t), :]).astype(BF16)
        mirror(aoo)
        own_copy().start()
        slot(3)
        for t in range(parts):
            cross_copy(t).wait_recv()
        for t in range(parts):
            aop[rows_at((t + 1) % parts), rows_at(t)] = ar[t].T

    def a_drain():
        for t in range(parts):
            cross_copy(t).wait_send()
        own_copy().wait_send()

    def poly(lin, acc):
        return (COEF_B * lin.astype(F32) + COEF_C * acc.astype(BF16).astype(F32)).astype(BF16)

    def renew(old, upd):
        return (COEF_A * old.astype(F32) + upd.astype(BF16).astype(F32)).astype(BF16)

    def ns_step(pair, parity):
        x, y, xn = xo[parity], xp[parity], xo[1 - parity]

        def slot(s):
            for (t, u), fns in tasks.items():
                if u == s and t % 2 == parity and t < NS_STEPS - 1:
                    def run(fns=fns):
                        for fn in fns:
                            fn()
                    pl.when(pair == t // 2)(run)

        def wait():
            if parity == 0:
                @pl.when(pair == 0)
                def _():
                    gath[0].finish()
                    gath[0].drain()

                @pl.when(pair > 0)
                def _():
                    x_wait(0)
            else:
                x_wait(1)

        grams(parity, slot, wait)
        for i in range(parts):
            sq = dot_nt(aoo[rows_at(i), :], aoo[i * blk:, :]) + dot_nt(aop[rows_at(i), :], aop[i * blk:, :])
            bo[rows_at(i), i * blk:] = poly(aoo[rows_at(i), i * blk:], sq)
        slot(4)
        own_copy().wait_recv()
        bp[...] = poly(aop[...], dot_nn(aoo[...], aop[...]) + dot_nn(aop[...], app[...]))
        mirror(bo)
        a_drain()
        for n in range(3):
            slot(5 + n)
            cols = pl.ds(n * third, third)
            xn[:, cols] = renew(x[:, cols], dot_nn(bo[...], x[:, cols]) + dot_nn(bp[...], y[:, cols]))
            x_copy(1 - parity, n).start()

    def ns_pair(pair, carry):
        ns_step(pair, 0)
        ns_step(pair, 1)
        return carry

    lax.fori_loop(0, NS_STEPS // 2, ns_pair, 0)

    def last_slot(s):
        for fn in tasks.get((NS_STEPS - 1, s), []):
            fn()

    grams(0, last_slot, lambda: x_wait(0))
    own_copy().wait_recv()
    top = pl.ds(0, sc['own'][0].shape[1])
    bo[top, :] = poly(aoo[top, :], dot_nt(aoo[top, :], aoo[...]) + dot_nt(aop[top, :], aop[...]))
    bp[top, :] = poly(aop[top, :], dot_nn(aoo[top, :], aop[...]) + dot_nn(aop[top, :], app[...]))
    a_drain()
    sc['oa'][...] = renew(xo[0][top, :], dot_nn(bo[top, :], xo[0][...]) + dot_nn(bp[top, :], xp[0][...]))
    out_copy(0, 1, sc['oa']).start()

    for k in (1, 2):
        gath[k].finish()
        gath[k].drain()
    bu = sc['bu']
    up_rows, down_rows = sc['own'][1].shape[1], sc['own'][2].shape[1]
    up_send, down_send = sc['up_send'], sc['down_send']
    up_copy = remote(up_send, sc['ou'], sc['osend'].at[0], sc['orecv'].at[0], place.partner)
    down_copy = remote(down_send, sc['od'], sc['osend'].at[1], sc['orecv'].at[1], place.partner)
    half_wide = wide // 2

    @pl.when(core == 0)
    def _():
        def step(it, carry):
            bu[0] = dot_tn(tall[...], tall[...]).astype(BF16)
            bu[1] = poly(bu[0], dot_nn(bu[0], bu[0]))
            for n in (0, 1):
                rows = pl.ds(n * half_wide, half_wide)
                tall[rows, :] = renew(tall[rows, :], dot_nn(tall[rows, :], bu[1]))
            return carry
        lax.fori_loop(0, NS_STEPS - 1, step, 0)
        bu[0] = dot_tn(tall[...], tall[...]).astype(BF16)
        bu[1] = poly(bu[0], dot_nn(bu[0], bu[0]))
        other = tall[half_wide:half_wide + up_rows, :]
        up_send[...] = renew(other, dot_nn(other, bu[1]))
        up_copy.start()
        own = tall[0:up_rows, :]
        sc['ou'][...] = renew(own, dot_nn(own, bu[1]))
        out_copy(1, 1, sc['ou']).start()
        down_copy.wait_recv()
        out_copy(2, 1, sc['od']).start()
        up_copy.wait_send()

    @pl.when(core == 1)
    def _():
        def step(it, carry):
            bu[0] = dot_nt(xd[...], xd[...]).astype(BF16)
            bu[1] = poly(bu[0], dot_nn(bu[0], bu[0]))
            for n in (0, 1):
                cols = pl.ds(n * half_wide, half_wide)
                xd[:, cols] = renew(xd[:, cols], dot_nn(bu[1], xd[:, cols]))
            return carry
        lax.fori_loop(0, NS_STEPS - 1, step, 0)
        bu[0] = dot_nt(xd[...], xd[...]).astype(BF16)

        def rows_of(which):
            rows = pl.ds(which * (small // 2), down_rows)
            part = poly(bu[0, rows, :], dot_nn(bu[0, rows, :], bu[0]))
            return renew(xd[rows, :], dot_nn(part, xd[...]))
        down_send[...] = rows_of(1)
        down_copy.start()
        sc['od'][...] = rows_of(0)
        out_copy(2, 1, sc['od']).start()
        up_copy.wait_recv()
        out_copy(1, 1, sc['ou']).start()
        down_copy.wait_send()

    for k in range(3):
        scat[k].drain()
    norm_drain(0)
    norm_drain(1)
    for k in range(3):
        out_copy(k, 0, sc['mom'][k]).wait()
        out_copy(k, 1, sc[('oa', 'ou', 'od')[k]]).wait()


def results_kernel(scales, *refs):
    for k in range(3):
        mom, ortho, master = refs[k], refs[3 + k], refs[6 + k]
        mom_out, master_out, weight_out = refs[9 + 3 * k:12 + 3 * k]
        mom_out[...] = mom[...]
        old = master[...]
        new = old - LEARN_RATE * (scales[k] * ortho[...].astype(F32) + WEIGHT_DECAY * old)
        master_out[...] = new
        weight_out[...] = new.astype(BF16)


def solution(mesh):
    group = mesh.shape['data']
    chips = group // 2
    pieces = chips - 1
    grad_spec = P(('stage', 'data'), None, None, None)
    row_spec = P('stage', 'data', None)

    def step_local(*arrays):
        grads = [arrays[3 * k].reshape(arrays[3 * k].shape[2:]) for k in range(3)]
        moms = [arrays[3 * k + 1].reshape(arrays[3 * k + 1].shape[1:]) for k in range(3)]
        masters = [arrays[3 * k + 2].reshape(arrays[3 * k + 2].shape[1:]) for k in range(3)]
        shapes = [m.shape for m in moms]
        size = grads[0].shape[0]
        wide, small = grads[1].shape
        dma = pltpu.SemaphoreType.DMA
        names, scratch = [], []

        def add(name, item):
            names.append(name)
            scratch.append(item)

        for k, (rows, cols) in enumerate(shapes):
            add(('own', k), pltpu.VMEM((chips, rows, cols), F32))
            add(('pair', k), pltpu.VMEM((chips, rows, cols), F32))
            add(('ring', k), pltpu.VMEM((2, chips // 2, rows, cols), F32))
            add(('mom', k), pltpu.VMEM((rows, cols), F32))
        half = size // 2
        for name in ('xo', 'xp'):
            add((name, 0), pltpu.VMEM((half, size), BF16))
            add((name, 1), pltpu.VMEM((half, size), BF16))
        for name in ('aoo', 'aop', 'app', 'bo', 'bp'):
            add(name, pltpu.VMEM((half, half), BF16))
        add('ar', pltpu.VMEM((3, half // 3, half // 3), BF16))
        add('tall', pltpu.VMEM((wide, small), BF16))
        add('xd', pltpu.VMEM((small, wide), BF16))
        add('bu', pltpu.VMEM((2, small, small), BF16))
        for name, k in (('oa', 0), ('ou', 1), ('od', 2), ('up_send', 1), ('down_send', 2)):
            add(name, pltpu.VMEM(shapes[k], BF16))
        add(('norm', 0), pltpu.VMEM((group, 8, 128), F32))
        add(('norm', 1), pltpu.VMEM((group, 16, 128), F32))
        for name, shape in (('load', (3, chips)), ('psend', (3, chips)), ('precv', (3, chips)), ('rsend', (3, 2, pieces)), ('rrecv', (3, 2, pieces)),
                            ('gsend', (3, 2, pieces)), ('grecv', (3, 2, pieces)), ('fsend', (3, 2, chips)), ('frecv', (3, 2, chips)),
                            ('nsend', (2, group)), ('nrecv', (2, group)), ('insem', (3,)), ('outsem', (6,)), ('asend', (4,)), ('arecv', (4,)),
                            ('xsend', (3,)), ('xrecv', (3,)), ('osend', (2,)), ('orecv', (2,))):
            add(name, dma(shape))

        def body(*refs):
            sc = {}
            for name, ref in zip(names, refs[12:]):
                if isinstance(name, tuple):
                    sc.setdefault(name[0], []).append(ref)
                else:
                    sc[name] = ref
            kernel(group, refs[0:3], refs[3:6], refs[6:12], sc)

        anywhere = pl.BlockSpec(memory_space=pl.ANY)
        part_shape = []
        for shape in shapes:
            part_shape += [jax.ShapeDtypeStruct(shape, F32), jax.ShapeDtypeStruct(shape, BF16)]
        parts = pl.pallas_call(
            body,
            out_shape=tuple(part_shape),
            in_specs=[anywhere] * 6,
            out_specs=tuple([anywhere] * 6),
            scratch_shapes=scratch,
            compiler_params=pltpu.CompilerParams(collective_id=0, has_side_effects=True, vmem_limit_bytes=64 * 1024 * 1024 - 65536),
            name='muon',
        )(*grads, *moms)
        scales = [0.2 * math.sqrt(max(g.shape)) for g in grads]
        out_shape = []
        for shape in shapes:
            out_shape += [jax.ShapeDtypeStruct(shape, F32), jax.ShapeDtypeStruct(shape, F32), jax.ShapeDtypeStruct(shape, BF16)]
        vmem = pl.BlockSpec(memory_space=pltpu.VMEM)
        results = pl.pallas_call(
            functools.partial(results_kernel, scales),
            out_shape=tuple(out_shape),
            in_specs=[vmem] * 9,
            out_specs=tuple([vmem] * 9),
            name='results',
        )(*parts[0::2], *parts[1::2], *masters)
        return tuple(r[None] for r in results)

    in_specs = (grad_spec, row_spec, row_spec) * 3
    out_specs = (row_spec,) * 9
    return jax.shard_map(step_local, mesh=mesh, in_specs=in_specs, out_specs=out_specs, check_vma=False)
```

```python
import functools
import math
import jax
import jax.numpy as jnp
from jax import lax
from jax.experimental import pallas as pl
from jax.experimental.pallas import tpu as pltpu
from jax.sharding import PartitionSpec as P

MOMENTUM = 0.95
LEARN_RATE = 0.25
WEIGHT_DECAY = 0.2
EPSILON = 1e-7
COEF_A = 3.4445
COEF_B = -4.7750
COEF_C = 2.0315
NS_STEPS = 5
F32 = jnp.float32
BF16 = jnp.bfloat16


def dot_nn(a, b):
    return lax.dot_general(a, b, (((1,), (0,)), ((), ())), preferred_element_type=F32)


def dot_tn(a, b):
    return lax.dot_general(a, b, (((0,), (0,)), ((), ())), preferred_element_type=F32)


def dot_nt(a, b):
    return lax.dot_general(a, b, (((1,), (1,)), ((), ())), preferred_element_type=F32)


def remote(src, dst, send_sem, recv_sem, dev):
    return pltpu.make_async_remote_copy(
        src_ref=src, dst_ref=dst, send_sem=send_sem, recv_sem=recv_sem,
        device_id={'data': dev}, device_id_type=pl.DeviceIdType.MESH)


def ds(start, size, mult):
    return pl.ds(pl.multiple_of(start, mult), size)


class Place:
    def __init__(self, group):
        self.group = group
        self.chips = group // 2
        self.me = lax.axis_index('data')
        self.chip = self.me // 2
        self.core = self.me % 2
        self.partner = self.chip * 2 + (1 - self.core)

    def at(self, offset):
        return lax.rem(self.chip + offset + self.chips, self.chips)

    def next(self, way):
        return self.at(1 if way == 0 else -1) * 2 + self.core


class Scatter:
    def __init__(self, place, grad, own, pair, ring, load, psend, precv, rsend, rrecv):
        self.pl, self.grad, self.own, self.pair, self.ring = place, grad, own, pair, ring
        self.load, self.psend, self.precv, self.rsend, self.rrecv = load, psend, precv, rsend, rrecv
        self.rows = own.shape[1]
        self.half_rows = self.rows // 2
        self.n = place.chips
        self.pieces = self.n - 1

    def order(self):
        far = self.n // 2
        order = [far]
        for d in range(far - 1, 0, -1):
            order += [d, self.n - d]
        return order + [0]

    def load_copy(self, d):
        row = (self.pl.at(d) * 2 + self.pl.core) * self.rows
        return pltpu.make_async_copy(self.grad.at[ds(row, self.rows, 32), :], self.own.at[d], self.load.at[d])

    def pair_copy(self, d):
        row = (self.pl.at(d) * 2 + (1 - self.pl.core)) * self.rows
        return remote(self.grad.at[ds(row, self.rows, 32), :], self.pair.at[d], self.psend.at[d], self.precv.at[d], self.pl.partner)

    def start(self):
        for d in self.order():
            self.pair_copy(d).start()
            self.load_copy(d).start()

    def arrive(self, d):
        self.load_copy(d).wait()
        self.pair_copy(d).wait_recv()

    def spot(self, way, q):
        dist = self.n // 2 - (q + 1) // 2
        half = way if q % 2 == 0 else 1 - way
        return dist, (dist if way == 0 else (self.n - dist) % self.n), pl.ds(half * self.half_rows, self.half_rows)

    def ring_copy(self, way, q):
        dist, d, rows = self.spot(way, q)
        return remote(self.own.at[d, rows, :], self.ring.at[way, dist - 1, rows, :], self.rsend.at[way, q], self.rrecv.at[way, q], self.pl.next(way))

    def step(self, q):
        for way in (0, 1):
            dist, d, rows = self.spot(way, q)
            if q % 2 == 1 or (q == 0 and way == 0):
                self.arrive(d)
            total = self.own[d, rows, :] + self.pair[d, rows, :]
            if q >= 2:
                self.ring_copy(way, q - 2).wait_recv()
                total = total + self.ring[way, dist, rows, :]
            self.own[d, rows, :] = total
            self.ring_copy(way, q).start()

    def total(self):
        self.arrive(0)
        for way in (0, 1):
            for q in (self.pieces - 2, self.pieces - 1):
                self.ring_copy(way, q).wait_recv()
        return (self.own[0] + self.pair[0]) + (self.ring[0, 0] + self.ring[1, 0])

    def drain(self):
        for d in range(self.n):
            self.pair_copy(d).wait_send()
        for way in (0, 1):
            for q in range(self.pieces):
                self.ring_copy(way, q).wait_send()


class Gather:
    def __init__(self, place, full, other, rows, to, rsend, rrecv, fsend, frecv):
        self.pl, self.full, self.other, self.rows, self.to = place, full, other, rows, to
        self.rsend, self.rrecv, self.fsend, self.frecv = rsend, rrecv, fsend, frecv
        self.half_rows = rows // 2
        self.n = place.chips
        self.pieces = self.n - 1

    def rows_of(self, way, q, lag):
        hop = q // 2 + lag
        slot = 0 if hop == 0 else min(2 * hop - 1 + way, self.n - 1)
        half = way if q % 2 == 0 else 1 - way
        return pl.ds(slot * self.rows + half * self.half_rows, self.half_rows)

    def ring_copy(self, way, q):
        return remote(self.full.at[self.rows_of(way, q, 0), :], self.full.at[self.rows_of(way, q, 1), :],
                      self.rsend.at[way, q], self.rrecv.at[way, q], self.pl.next(way))

    def forward(self, way, q):
        rows = self.rows_of(way, q, 1)
        return remote(self.full.at[rows, :], self.other.at[rows, :], self.fsend.at[way, q], self.frecv.at[way, q], self.pl.partner)

    def forward_own(self):
        rows = pl.ds(0, self.rows)
        return remote(self.full.at[rows, :], self.other.at[rows, :], self.fsend.at[0, self.pieces], self.frecv.at[0, self.pieces], self.pl.partner)

    def sending(self, fn):
        if self.to is None:
            fn()
        else:
            pl.when(self.pl.core != self.to)(fn)

    def step(self, q):
        if q == 0:
            for k in (0, 1):
                for way in (0, 1):
                    self.ring_copy(way, k).start()
            self.sending(lambda: self.forward_own().start())
        else:
            for way in (0, 1):
                self.ring_copy(way, q - 1).wait_recv()
                if q + 1 < self.pieces:
                    self.ring_copy(way, q + 1).start()

            def hand_on():
                for way in (0, 1):
                    self.forward(way, q - 1).start()
            self.sending(hand_on)

    def steps(self):
        return self.pieces + 1

    def finish(self):
        def run():
            self.forward_own().wait_recv()
            for way in (0, 1):
                for q in range(self.pieces):
                    self.forward(way, q).wait_recv()
        if self.to is None:
            run()
        else:
            pl.when(self.pl.core == self.to)(run)

    def drain(self):
        for way in (0, 1):
            for q in range(self.pieces):
                self.ring_copy(way, q).wait_send()

        def run():
            self.forward_own().wait_send()
            for way in (0, 1):
                for q in range(self.pieces):
                    self.forward(way, q).wait_send()
        self.sending(run)


def squares(mat):
    sq = mat * mat
    rows, cols = mat.shape
    acc = sq[0:8]
    for i in range(1, rows // 8):
        acc = acc + sq[8 * i:8 * i + 8]
    out = acc[:, 0:128]
    for j in range(1, cols // 128):
        out = out + acc[:, 128 * j:128 * j + 128]
    return out


def total_norm(ref, top):
    acc = ref[0, top:top + 8]
    for i in range(1, ref.shape[0]):
        acc = acc + ref[i, top:top + 8]
    total = jnp.sum(jnp.sum(acc, axis=1, keepdims=True), axis=0, keepdims=True)
    return jnp.sqrt(total) + EPSILON


def kernel(group, grads, moms, outs, sc):
    place = Place(group)
    core, chip = place.core, place.chip
    chips = place.chips
    pieces = chips - 1
    barrier = pltpu.get_barrier_semaphore()
    for dev in (place.partner, place.next(0), place.next(1)):
        pl.semaphore_signal(barrier, inc=1, device_id={'data': dev}, device_id_type=pl.DeviceIdType.MESH)
    pl.semaphore_wait(barrier, 3)

    scat = [Scatter(place, grads[k], sc['own'][k], sc['pair'][k], sc['ring'][k], sc['load'].at[k], sc['psend'].at[k], sc['precv'].at[k],
                    sc['rsend'].at[k], sc['rrecv'].at[k]) for k in range(3)]
    xs = sc['x']
    size = xs[0].shape[0]
    half = size // 2
    xd, tall = sc['xd'], sc['tall']
    small, wide = xd.shape
    fulls = [xs[0].at[pl.ds(0, half), :], tall.at[pl.ds(0, wide // 2), :], xd.at[pl.ds(0, small // 2), :]]
    others = [xs[0].at[pl.ds(half, half), :], tall.at[pl.ds(wide // 2, wide // 2), :], xd.at[pl.ds(small // 2, small // 2), :]]
    gath = [Gather(place, fulls[k], others[k], sc['own'][k].shape[1], (None, 0, 1)[k], sc['gsend'].at[k], sc['grecv'].at[k], sc['fsend'].at[k], sc['frecv'].at[k])
            for k in range(3)]

    scat[0].start()
    in_copies = []
    for k in range(3):
        in_copies.append(pltpu.make_async_copy(moms[k], sc['mom'][k], sc['insem'].at[k]))
        in_copies[k].start()
    scat[1].start()
    scat[2].start()

    def out_copy(k, j, ref):
        return pltpu.make_async_copy(ref, outs[2 * k + j], sc['outsem'].at[2 * k + j])

    def momentum(k):
        in_copies[k].wait()
        mat = MOMENTUM * sc['mom'][k][...] + scat[k].total() * (1.0 / group)
        sc['mom'][k][...] = mat
        out_copy(k, 0, sc['mom'][k]).start()
        return squares(mat)

    def norm_copy(idx, i):
        ref = sc['norm'][idx]
        dev = lax.rem(place.me + i, group)
        return remote(ref.at[0], ref.at[i], sc['nsend'].at[idx, i], sc['nrecv'].at[idx, i], dev)

    def norm_send(idx):
        for i in range(1, group):
            norm_copy(idx, i).start()

    def norm_wait(idx):
        for i in range(1, group):
            norm_copy(idx, i).wait_recv()

    def norm_drain(idx):
        for i in range(1, group):
            norm_copy(idx, i).wait_send()

    def write_x(k, norm):
        rows = sc['own'][k].shape[1]
        fulls[k][0:rows, :] = (sc['mom'][k][...] / norm).astype(BF16)

    for q in range(pieces):
        scat[0].step(q)
    sc['norm'][0][0] = momentum(0)
    norm_send(0)
    for q in (0, 1):
        for k in (1, 2):
            scat[k].step(q)
    norm_wait(0)
    write_x(0, total_norm(sc['norm'][0], 0))
    for q in range(gath[0].steps()):
        gath[0].step(q)
        if q + 2 == pieces:
            for k in (1, 2):
                scat[k].step(2)

    tasks = {}

    def background(it, slot, fn):
        tasks.setdefault((it, slot), []).append(fn)

    def ud_momentum():
        sc['norm'][1][0, 0:8] = momentum(1)
        sc['norm'][1][0, 8:16] = momentum(2)
        norm_send(1)

    def ud_write():
        norm_wait(1)
        write_x(1, total_norm(sc['norm'][1], 0))
        write_x(2, total_norm(sc['norm'][1], 8))

    def both(parts, q):
        def run():
            parts[1].step(q)
            parts[2].step(q)
        return run

    background(0, 0, both(scat, 3))
    for q, place_at in ((4, (0, 3)), (5, (0, 8)), (6, (1, 2))):
        background(*place_at, both(scat, q))
    background(2, 1, ud_momentum)
    background(2, 6, ud_write)
    times = ((2, 6), (3, 2), (3, 3), (3, 5), (3, 9), (4, 1), (4, 3), (4, 4))
    for q in range(gath[1].steps()):
        background(*times[q], both(gath, q))

    grids, b, ar, qacc = sc['a'], sc['b'], sc['ar'], sc['qacc']
    parts = 3
    blk = half // parts
    tiles = tuple((n * blk, blk) for n in range(2 * parts))

    def rows_at(i):
        return pl.ds(i * blk, blk)

    def far_at(i):
        return pl.ds(half + i * blk, blk)

    def cross_copy(way, t):
        return remote(grids[way].at[rows_at(t), far_at((t + 1) % parts)], ar.at[t], sc['asend'].at[way, t], sc['arecv'].at[way, t], place.partner)

    def own_copy(way, i):
        width = half - i * blk
        return remote(grids[way].at[rows_at(i), pl.ds(i * blk, width)], grids[way].at[far_at(i), pl.ds(half + i * blk, width)],
                      sc['asend'].at[way, parts + i], sc['arecv'].at[way, parts + i], place.partner)

    def x_copy(way, n):
        cols = pl.ds(*tiles[n])
        return remote(xs[way].at[pl.ds(0, half), cols], xs[way].at[pl.ds(half, half), cols], sc['xsend'].at[n], sc['xrecv'].at[n], place.partner)

    def x_wait(way):
        for n in range(len(tiles)):
            x_copy(way, n).wait_recv()
            x_copy(way, n).wait_send()

    def mirror(ref, at):
        for i in range(parts):
            for j in range(i + 1, parts):
                ref[at(j), at(i)] = ref[at(i), at(j)].T

    def grams(way, slot, wait):
        x, a = xs[way], grids[way]
        slot(0)
        for i in range(parts):
            a[rows_at(i), i * blk:half] = dot_nt(x[rows_at(i), :], x[i * blk:half, :]).astype(BF16)
        for i in range(parts):
            own_copy(way, i).start()
        slot(1)
        wait()
        for t in range(parts):
            a[rows_at(t), far_at((t + 1) % parts)] = dot_nt(x[rows_at(t), :], x[far_at((t + 1) % parts), :]).astype(BF16)
        for t in range(parts):
            cross_copy(way, t).start()
        slot(2)
        mirror(a, rows_at)
        for t in range(parts):
            a[rows_at(t), far_at(t)] = dot_nt(x[rows_at(t), :], x[far_at(t), :]).astype(BF16)

    def crosses(way):
        a = grids[way]
        for t in range(parts):
            own_copy(way, t).wait_recv()
            cross_copy(way, t).wait_recv()
        for t in range(parts):
            a[rows_at((t + 1) % parts), far_at(t)] = ar[t].T
        mirror(a, far_at)

    def a_drain(way):
        for t in range(parts):
            own_copy(way, t).wait_send()
            cross_copy(way, t).wait_send()

    def poly(lin, acc):
        return (COEF_B * lin.astype(F32) + COEF_C * acc.astype(BF16).astype(F32)).astype(BF16)

    def renew(old, upd):
        return (COEF_A * old.astype(F32) + upd.astype(BF16).astype(F32)).astype(BF16)

    def ns_step(pair, parity):
        x, xn, a = xs[parity], xs[1 - parity], grids[parity]

        def slot(s):
            for (t, u), fns in tasks.items():
                if u == s and t % 2 == parity and t < NS_STEPS - 1:
                    def run(fns=fns):
                        for fn in fns:
                            fn()
                    pl.when(pair == t // 2)(run)

        def wait():
            if parity == 0:
                @pl.when(pair == 0)
                def _():
                    gath[0].finish()
                    gath[0].drain()

                @pl.when(pair > 0)
                def _():
                    x_wait(0)
            else:
                x_wait(1)

        grams(parity, slot, wait)
        for i in range(parts):
            qacc[rows_at(i), i * blk:] = dot_nt(a[rows_at(i), 0:half], a[i * blk:half, 0:half])
        slot(3)
        crosses(parity)
        for i in range(parts):
            sq = qacc[rows_at(i), i * blk:] + dot_nt(a[rows_at(i), half:], a[i * blk:half, half:])
            b[rows_at(i), i * blk:half] = poly(a[rows_at(i), i * blk:half], sq)
        slot(4)
        b[:, half:] = poly(a[0:half, half:], dot_nn(a[0:half, :], a[:, half:]))
        mirror(b, rows_at)
        a_drain(parity)
        for n, (left, width) in enumerate(tiles):
            slot(5 + n)
            cols = pl.ds(left, width)
            xn[0:half, cols] = renew(x[0:half, cols], dot_nn(b[...], x[:, cols]))
            x_copy(1 - parity, n).start()

    def ns_pair(pair, carry):
        ns_step(pair, 0)
        ns_step(pair, 1)
        return carry

    lax.fori_loop(0, NS_STEPS // 2, ns_pair, 0)

    def last_slot(s):
        for fn in tasks.get((NS_STEPS - 1, s), []):
            fn()

    grams(0, last_slot, lambda: x_wait(0))
    last_slot(3)
    crosses(0)
    a = grids[0]
    top = pl.ds(0, sc['own'][0].shape[1])
    b[top, 0:half] = poly(a[top, 0:half], dot_nt(a[top, :], a[0:half, :]))
    b[top, half:] = poly(a[top, half:], dot_nn(a[top, :], a[:, half:]))
    a_drain(0)
    sc['oa'][...] = renew(xs[0][top, :], dot_nn(b[top, :], xs[0][...]))
    out_copy(0, 1, sc['oa']).start()
    last_slot(4)

    for k in (1, 2):
        gath[k].finish()
        gath[k].drain()
    bu = sc['bu']
    up_rows, down_rows = sc['own'][1].shape[1], sc['own'][2].shape[1]
    up_send, down_send = sc['up_send'], sc['down_send']
    up_copy = remote(up_send, sc['ou'], sc['osend'].at[0], sc['orecv'].at[0], place.partner)
    down_copy = remote(down_send, sc['od'], sc['osend'].at[1], sc['orecv'].at[1], place.partner)
    half_wide = wide // 2

    @pl.when(core == 0)
    def _():
        def step(it, carry):
            bu[0] = dot_tn(tall[...], tall[...]).astype(BF16)
            bu[1] = poly(bu[0], dot_nn(bu[0], bu[0]))
            for n in (0, 1):
                rows = pl.ds(n * half_wide, half_wide)
                tall[rows, :] = renew(tall[rows, :], dot_nn(tall[rows, :], bu[1]))
            return carry
        lax.fori_loop(0, NS_STEPS - 1, step, 0)
        bu[0] = dot_tn(tall[...], tall[...]).astype(BF16)
        bu[1] = poly(bu[0], dot_nn(bu[0], bu[0]))
        other = tall[half_wide:half_wide + up_rows, :]
        up_send[...] = renew(other, dot_nn(other, bu[1]))
        up_copy.start()
        own = tall[0:up_rows, :]
        sc['ou'][...] = renew(own, dot_nn(own, bu[1]))
        out_copy(1, 1, sc['ou']).start()
        down_copy.wait_recv()
        out_copy(2, 1, sc['od']).start()
        up_copy.wait_send()

    @pl.when(core == 1)
    def _():
        def step(it, carry):
            bu[0] = dot_nt(xd[...], xd[...]).astype(BF16)
            bu[1] = poly(bu[0], dot_nn(bu[0], bu[0]))
            for n in (0, 1):
                cols = pl.ds(n * half_wide, half_wide)
                xd[:, cols] = renew(xd[:, cols], dot_nn(bu[1], xd[:, cols]))
            return carry
        lax.fori_loop(0, NS_STEPS - 1, step, 0)
        bu[0] = dot_nt(xd[...], xd[...]).astype(BF16)

        def rows_of(which):
            rows = pl.ds(which * (small // 2), down_rows)
            part = poly(bu[0, rows, :], dot_nn(bu[0, rows, :], bu[0]))
            return renew(xd[rows, :], dot_nn(part, xd[...]))
        down_send[...] = rows_of(1)
        down_copy.start()
        sc['od'][...] = rows_of(0)
        out_copy(2, 1, sc['od']).start()
        up_copy.wait_recv()
        out_copy(1, 1, sc['ou']).start()
        down_copy.wait_send()

    for k in range(3):
        scat[k].drain()
    norm_drain(0)
    norm_drain(1)
    for k in range(3):
        out_copy(k, 0, sc['mom'][k]).wait()
        out_copy(k, 1, sc[('oa', 'ou', 'od')[k]]).wait()


def results_kernel(scales, *refs):
    for k in range(3):
        mom, ortho, master = refs[k], refs[3 + k], refs[6 + k]
        mom_out, master_out, weight_out = refs[9 + 3 * k:12 + 3 * k]
        mom_out[...] = mom[...]
        old = master[...]
        new = old - LEARN_RATE * (scales[k] * ortho[...].astype(F32) + WEIGHT_DECAY * old)
        master_out[...] = new
        weight_out[...] = new.astype(BF16)


def solution(mesh):
    group = mesh.shape['data']
    chips = group // 2
    pieces = chips - 1
    grad_spec = P(('stage', 'data'), None, None, None)
    row_spec = P('stage', 'data', None)

    def step_local(*arrays):
        grads = [arrays[3 * k].reshape(arrays[3 * k].shape[2:]) for k in range(3)]
        moms = [arrays[3 * k + 1].reshape(arrays[3 * k + 1].shape[1:]) for k in range(3)]
        masters = [arrays[3 * k + 2].reshape(arrays[3 * k + 2].shape[1:]) for k in range(3)]
        shapes = [m.shape for m in moms]
        size = grads[0].shape[0]
        wide, small = grads[1].shape
        dma = pltpu.SemaphoreType.DMA
        names, scratch = [], []

        def add(name, item):
            names.append(name)
            scratch.append(item)

        for k, (rows, cols) in enumerate(shapes):
            add(('own', k), pltpu.VMEM((chips, rows, cols), F32))
            add(('pair', k), pltpu.VMEM((chips, rows, cols), F32))
            add(('ring', k), pltpu.VMEM((2, chips // 2, rows, cols), F32))
            add(('mom', k), pltpu.VMEM((rows, cols), F32))
        half = size // 2
        add(('x', 0), pltpu.VMEM((size, size), BF16))
        add(('x', 1), pltpu.VMEM((size, size), BF16))
        add(('a', 0), pltpu.VMEM((size, size), BF16))
        add(('a', 1), pltpu.VMEM((size, size), BF16))
        add('qacc', pltpu.VMEM((half, half), F32))
        add('b', pltpu.VMEM((half, size), BF16))
        add('ar', pltpu.VMEM((3, half // 3, half // 3), BF16))
        add('tall', pltpu.VMEM((wide, small), BF16))
        add('xd', pltpu.VMEM((small, wide), BF16))
        add('bu', pltpu.VMEM((2, small, small), BF16))
        for name, k in (('oa', 0), ('ou', 1), ('od', 2), ('up_send', 1), ('down_send', 2)):
            add(name, pltpu.VMEM(shapes[k], BF16))
        add(('norm', 0), pltpu.VMEM((group, 8, 128), F32))
        add(('norm', 1), pltpu.VMEM((group, 16, 128), F32))
        for name, shape in (('load', (3, chips)), ('psend', (3, chips)), ('precv', (3, chips)), ('rsend', (3, 2, pieces)), ('rrecv', (3, 2, pieces)),
                            ('gsend', (3, 2, pieces)), ('grecv', (3, 2, pieces)), ('fsend', (3, 2, chips)), ('frecv', (3, 2, chips)),
                            ('nsend', (2, group)), ('nrecv', (2, group)), ('insem', (3,)), ('outsem', (6,)), ('asend', (2, 6)), ('arecv', (2, 6)),
                            ('xsend', (6,)), ('xrecv', (6,)), ('osend', (2,)), ('orecv', (2,))):
            add(name, dma(shape))

        def body(*refs):
            sc = {}
            for name, ref in zip(names, refs[12:]):
                if isinstance(name, tuple):
                    sc.setdefault(name[0], []).append(ref)
                else:
                    sc[name] = ref
            kernel(group, refs[0:3], refs[3:6], refs[6:12], sc)

        anywhere = pl.BlockSpec(memory_space=pl.ANY)
        part_shape = []
        for shape in shapes:
            part_shape += [jax.ShapeDtypeStruct(shape, F32), jax.ShapeDtypeStruct(shape, BF16)]
        parts = pl.pallas_call(
            body,
            out_shape=tuple(part_shape),
            in_specs=[anywhere] * 6,
            out_specs=tuple([anywhere] * 6),
            scratch_shapes=scratch,
            compiler_params=pltpu.CompilerParams(collective_id=0, has_side_effects=True, vmem_limit_bytes=64 * 1024 * 1024 - 65536),
            name='muon',
        )(*grads, *moms)
        scales = [0.2 * math.sqrt(max(g.shape)) for g in grads]
        out_shape = []
        for shape in shapes:
            out_shape += [jax.ShapeDtypeStruct(shape, F32), jax.ShapeDtypeStruct(shape, F32), jax.ShapeDtypeStruct(shape, BF16)]
        vmem = pl.BlockSpec(memory_space=pltpu.VMEM)
        results = pl.pallas_call(
            functools.partial(results_kernel, scales),
            out_shape=tuple(out_shape),
            in_specs=[vmem] * 9,
            out_specs=tuple([vmem] * 9),
            name='results',
        )(*parts[0::2], *parts[1::2], *masters)
        return tuple(r[None] for r in results)

    in_specs = (grad_spec, row_spec, row_spec) * 3
    out_specs = (row_spec,) * 9
    return jax.shard_map(step_local, mesh=mesh, in_specs=in_specs, out_specs=out_specs, check_vma=False)
```

```python
import functools
import math
import jax
import jax.numpy as jnp
from jax import lax
from jax.experimental import pallas as pl
from jax.experimental.pallas import tpu as pltpu
from jax.sharding import PartitionSpec as P

MOMENTUM = 0.95
LEARN_RATE = 0.25
WEIGHT_DECAY = 0.2
EPSILON = 1e-7
COEF_A = 3.4445
COEF_B = -4.7750
COEF_C = 2.0315
NS_STEPS = 5
F32 = jnp.float32
BF16 = jnp.bfloat16


def dot_nn(a, b):
    return lax.dot_general(a, b, (((1,), (0,)), ((), ())), preferred_element_type=F32)


def dot_tn(a, b):
    return lax.dot_general(a, b, (((0,), (0,)), ((), ())), preferred_element_type=F32)


def dot_nt(a, b):
    return lax.dot_general(a, b, (((1,), (1,)), ((), ())), preferred_element_type=F32)


def remote(src, dst, send_sem, recv_sem, dev):
    return pltpu.make_async_remote_copy(
        src_ref=src, dst_ref=dst, send_sem=send_sem, recv_sem=recv_sem,
        device_id={'data': dev}, device_id_type=pl.DeviceIdType.MESH)


def ds(start, size, mult):
    return pl.ds(pl.multiple_of(start, mult), size)


class Place:
    def __init__(self, group):
        self.group = group
        self.chips = group // 2
        self.me = lax.axis_index('data')
        self.chip = self.me // 2
        self.core = self.me % 2
        self.partner = self.chip * 2 + (1 - self.core)

    def at(self, offset):
        return lax.rem(self.chip + offset + self.chips, self.chips)

    def next(self, way):
        return self.at(1 if way == 0 else -1) * 2 + self.core


class Scatter:
    def __init__(self, place, grad, own, pair, ring, load, psend, precv, rsend, rrecv):
        self.pl, self.grad, self.own, self.pair, self.ring = place, grad, own, pair, ring
        self.load, self.psend, self.precv, self.rsend, self.rrecv = load, psend, precv, rsend, rrecv
        self.rows = own.shape[1]
        self.half_rows = self.rows // 2
        self.n = place.chips
        self.pieces = self.n - 1

    def order(self):
        far = self.n // 2
        order = [far]
        for d in range(far - 1, 0, -1):
            order += [d, self.n - d]
        return order + [0]

    def load_copy(self, d):
        row = (self.pl.at(d) * 2 + self.pl.core) * self.rows
        return pltpu.make_async_copy(self.grad.at[ds(row, self.rows, 32), :], self.own.at[d], self.load.at[d])

    def pair_copy(self, d):
        row = (self.pl.at(d) * 2 + (1 - self.pl.core)) * self.rows
        return remote(self.grad.at[ds(row, self.rows, 32), :], self.pair.at[d], self.psend.at[d], self.precv.at[d], self.pl.partner)

    def start(self):
        for d in self.order():
            self.pair_copy(d).start()
            self.load_copy(d).start()

    def arrive(self, d):
        self.load_copy(d).wait()
        self.pair_copy(d).wait_recv()

    def spot(self, way, q):
        dist = self.n // 2 - (q + 1) // 2
        half = way if q % 2 == 0 else 1 - way
        return dist, (dist if way == 0 else (self.n - dist) % self.n), pl.ds(half * self.half_rows, self.half_rows)

    def ring_copy(self, way, q):
        dist, d, rows = self.spot(way, q)
        return remote(self.own.at[d, rows, :], self.ring.at[way, dist - 1, rows, :], self.rsend.at[way, q], self.rrecv.at[way, q], self.pl.next(way))

    def step(self, q):
        for way in (0, 1):
            dist, d, rows = self.spot(way, q)
            if q % 2 == 1 or (q == 0 and way == 0):
                self.arrive(d)
            total = self.own[d, rows, :] + self.pair[d, rows, :]
            if q >= 2:
                self.ring_copy(way, q - 2).wait_recv()
                total = total + self.ring[way, dist, rows, :]
            self.own[d, rows, :] = total
            self.ring_copy(way, q).start()

    def total(self):
        self.arrive(0)
        for way in (0, 1):
            for q in (self.pieces - 2, self.pieces - 1):
                self.ring_copy(way, q).wait_recv()
        return (self.own[0] + self.pair[0]) + (self.ring[0, 0] + self.ring[1, 0])

    def drain(self):
        for d in range(self.n):
            self.pair_copy(d).wait_send()
        for way in (0, 1):
            for q in range(self.pieces):
                self.ring_copy(way, q).wait_send()


class Gather:
    def __init__(self, place, full, other, rows, to, rsend, rrecv, fsend, frecv):
        self.pl, self.full, self.other, self.rows, self.to = place, full, other, rows, to
        self.rsend, self.rrecv, self.fsend, self.frecv = rsend, rrecv, fsend, frecv
        self.half_rows = rows // 2
        self.n = place.chips
        self.pieces = self.n - 1

    def rows_of(self, way, q, lag):
        hop = q // 2 + lag
        slot = 0 if hop == 0 else min(2 * hop - 1 + way, self.n - 1)
        half = way if q % 2 == 0 else 1 - way
        return pl.ds(slot * self.rows + half * self.half_rows, self.half_rows)

    def ring_copy(self, way, q):
        return remote(self.full.at[self.rows_of(way, q, 0), :], self.full.at[self.rows_of(way, q, 1), :],
                      self.rsend.at[way, q], self.rrecv.at[way, q], self.pl.next(way))

    def forward(self, way, q):
        rows = self.rows_of(way, q, 1)
        return remote(self.full.at[rows, :], self.other.at[rows, :], self.fsend.at[way, q], self.frecv.at[way, q], self.pl.partner)

    def forward_own(self):
        rows = pl.ds(0, self.rows)
        return remote(self.full.at[rows, :], self.other.at[rows, :], self.fsend.at[0, self.pieces], self.frecv.at[0, self.pieces], self.pl.partner)

    def sending(self, fn):
        if self.to is None:
            fn()
        else:
            pl.when(self.pl.core != self.to)(fn)

    def step(self, q):
        if q == 0:
            for k in (0, 1):
                for way in (0, 1):
                    self.ring_copy(way, k).start()
            self.sending(lambda: self.forward_own().start())
        else:
            for way in (0, 1):
                self.ring_copy(way, q - 1).wait_recv()
                if q + 1 < self.pieces:
                    self.ring_copy(way, q + 1).start()

            def hand_on():
                for way in (0, 1):
                    self.forward(way, q - 1).start()
            self.sending(hand_on)

    def steps(self):
        return self.pieces + 1

    def finish(self):
        def run():
            self.forward_own().wait_recv()
            for way in (0, 1):
                for q in range(self.pieces):
                    self.forward(way, q).wait_recv()
        if self.to is None:
            run()
        else:
            pl.when(self.pl.core == self.to)(run)

    def drain(self):
        for way in (0, 1):
            for q in range(self.pieces):
                self.ring_copy(way, q).wait_send()

        def run():
            self.forward_own().wait_send()
            for way in (0, 1):
                for q in range(self.pieces):
                    self.forward(way, q).wait_send()
        self.sending(run)


def squares(mat):
    sq = mat * mat
    rows, cols = mat.shape
    acc = sq[0:8]
    for i in range(1, rows // 8):
        acc = acc + sq[8 * i:8 * i + 8]
    out = acc[:, 0:128]
    for j in range(1, cols // 128):
        out = out + acc[:, 128 * j:128 * j + 128]
    return out


def total_norm(ref, top):
    acc = ref[0, top:top + 8]
    for i in range(1, ref.shape[0]):
        acc = acc + ref[i, top:top + 8]
    total = jnp.sum(jnp.sum(acc, axis=1, keepdims=True), axis=0, keepdims=True)
    return jnp.sqrt(total) + EPSILON


def kernel(group, grads, moms, outs, sc):
    place = Place(group)
    core, chip = place.core, place.chip
    chips = place.chips
    pieces = chips - 1
    barrier = pltpu.get_barrier_semaphore()
    for dev in (place.partner, place.next(0), place.next(1)):
        pl.semaphore_signal(barrier, inc=1, device_id={'data': dev}, device_id_type=pl.DeviceIdType.MESH)
    pl.semaphore_wait(barrier, 3)

    scat = [Scatter(place, grads[k], sc['own'][k], sc['pair'][k], sc['ring'][k], sc['load'].at[k], sc['psend'].at[k], sc['precv'].at[k],
                    sc['rsend'].at[k], sc['rrecv'].at[k]) for k in range(3)]
    xs = sc['x']
    size = xs[0].shape[0]
    half = size // 2
    xd, tall = sc['xd'], sc['tall']
    small, wide = xd.shape
    fulls = [xs[0].at[pl.ds(0, half), :], tall.at[pl.ds(0, wide // 2), :], xd.at[pl.ds(0, small // 2), :]]
    others = [xs[0].at[pl.ds(half, half), :], tall.at[pl.ds(wide // 2, wide // 2), :], xd.at[pl.ds(small // 2, small // 2), :]]
    gath = [Gather(place, fulls[k], others[k], sc['own'][k].shape[1], (None, 0, 1)[k], sc['gsend'].at[k], sc['grecv'].at[k], sc['fsend'].at[k], sc['frecv'].at[k])
            for k in range(3)]

    scat[0].start()
    in_copies = []
    for k in range(3):
        in_copies.append(pltpu.make_async_copy(moms[k], sc['mom'][k], sc['insem'].at[k]))
        in_copies[k].start()
    scat[1].start()
    scat[2].start()

    def out_copy(k, j, ref):
        return pltpu.make_async_copy(ref, outs[2 * k + j], sc['outsem'].at[2 * k + j])

    def momentum(k):
        in_copies[k].wait()
        mat = MOMENTUM * sc['mom'][k][...] + scat[k].total() * (1.0 / group)
        sc['mom'][k][...] = mat
        out_copy(k, 0, sc['mom'][k]).start()
        return squares(mat)

    def norm_copy(idx, i):
        ref = sc['norm'][idx]
        dev = lax.rem(place.me + i, group)
        return remote(ref.at[0], ref.at[i], sc['nsend'].at[idx, i], sc['nrecv'].at[idx, i], dev)

    def norm_send(idx):
        for i in range(1, group):
            norm_copy(idx, i).start()

    def norm_wait(idx):
        for i in range(1, group):
            norm_copy(idx, i).wait_recv()

    def norm_drain(idx):
        for i in range(1, group):
            norm_copy(idx, i).wait_send()

    def write_x(k, norm):
        rows = sc['own'][k].shape[1]
        fulls[k][0:rows, :] = (sc['mom'][k][...] / norm).astype(BF16)

    for q in range(pieces):
        scat[0].step(q)
    sc['norm'][0][0] = momentum(0)
    norm_send(0)
    for q in (0, 1):
        for k in (1, 2):
            scat[k].step(q)
    norm_wait(0)
    write_x(0, total_norm(sc['norm'][0], 0))
    for q in range(gath[0].steps()):
        gath[0].step(q)
        if q + 2 == pieces:
            for k in (1, 2):
                scat[k].step(2)

    tasks = {}

    def background(it, slot, fn):
        tasks.setdefault((it, slot), []).append(fn)

    def ud_momentum():
        sc['norm'][1][0, 0:8] = momentum(1)
        sc['norm'][1][0, 8:16] = momentum(2)
        norm_send(1)

    def ud_write():
        norm_wait(1)
        write_x(1, total_norm(sc['norm'][1], 0))
        write_x(2, total_norm(sc['norm'][1], 8))

    def both(parts, q):
        def run():
            parts[1].step(q)
            parts[2].step(q)
        return run

    background(0, 0, both(scat, 3))
    for q, place_at in ((4, (0, 3)), (5, (0, 6)), (6, (1, 2))):
        background(*place_at, both(scat, q))
    background(2, 0, ud_momentum)
    background(2, 5, ud_write)
    times = ((2, 5), (3, 1), (3, 3), (3, 5), (3, 6), (4, 1), (4, 3), (4, 4))
    for q in range(gath[1].steps()):
        background(*times[q], both(gath, q))

    grids, b, ar, qacc = sc['a'], sc['b'], sc['ar'], sc['qacc']
    parts = 3
    blk = half // parts
    tiles = tuple((n * 2 * blk, 2 * blk) for n in range(parts))

    def rows_at(i):
        return pl.ds(i * blk, blk)

    def far_at(i):
        return pl.ds(half + i * blk, blk)

    def cross_copy(way, t):
        return remote(grids[way].at[rows_at(t), far_at((t + 1) % parts)], ar.at[t], sc['asend'].at[way, t], sc['arecv'].at[way, t], place.partner)

    def own_copy(way, i):
        width = half - i * blk
        return remote(grids[way].at[rows_at(i), pl.ds(i * blk, width)], grids[way].at[far_at(i), pl.ds(half + i * blk, width)],
                      sc['asend'].at[way, parts + i], sc['arecv'].at[way, parts + i], place.partner)

    def x_copy(way, n):
        cols = pl.ds(*tiles[n])
        return remote(xs[way].at[pl.ds(0, half), cols], xs[way].at[pl.ds(half, half), cols], sc['xsend'].at[n], sc['xrecv'].at[n], place.partner)

    def x_wait(way):
        for n in range(len(tiles)):
            x_copy(way, n).wait_recv()
            x_copy(way, n).wait_send()

    def mirror(ref, at):
        for i in range(parts):
            for j in range(i + 1, parts):
                ref[at(j), at(i)] = ref[at(i), at(j)].T

    def grams(way, slot, wait):
        x, a = xs[way], grids[way]
        slot(0)
        for i in range(parts):
            a[rows_at(i), i * blk:half] = dot_nt(x[rows_at(i), :], x[i * blk:half, :]).astype(BF16)
        for i in range(parts):
            own_copy(way, i).start()
        slot(1)
        wait()
        for t in range(parts):
            a[rows_at(t), far_at((t + 1) % parts)] = dot_nt(x[rows_at(t), :], x[far_at((t + 1) % parts), :]).astype(BF16)
        for t in range(parts):
            cross_copy(way, t).start()
        slot(2)
        mirror(a, rows_at)
        for t in range(parts):
            a[rows_at(t), far_at(t)] = dot_nt(x[rows_at(t), :], x[far_at(t), :]).astype(BF16)

    def crosses(way):
        a = grids[way]
        for t in range(parts):
            own_copy(way, t).wait_recv()
            cross_copy(way, t).wait_recv()
        for t in range(parts):
            a[rows_at((t + 1) % parts), far_at(t)] = ar[t].T
        mirror(a, far_at)

    def a_drain(way):
        for t in range(parts):
            own_copy(way, t).wait_send()
            cross_copy(way, t).wait_send()

    def poly(lin, acc):
        return (COEF_B * lin.astype(F32) + COEF_C * acc.astype(BF16).astype(F32)).astype(BF16)

    def renew(old, upd):
        return (COEF_A * old.astype(F32) + upd.astype(BF16).astype(F32)).astype(BF16)

    def ns_step(pair, parity):
        x, xn, a = xs[parity], xs[1 - parity], grids[parity]

        def slot(s):
            for (t, u), fns in tasks.items():
                if u == s and t % 2 == parity and t < NS_STEPS - 1:
                    def run(fns=fns):
                        for fn in fns:
                            fn()
                    pl.when(pair == t // 2)(run)

        def wait():
            if parity == 0:
                @pl.when(pair == 0)
                def _():
                    gath[0].finish()
                    gath[0].drain()

                @pl.when(pair > 0)
                def _():
                    x_wait(0)
            else:
                x_wait(1)

        grams(parity, slot, wait)
        for i in range(parts):
            qacc[rows_at(i), i * blk:] = dot_nt(a[rows_at(i), 0:half], a[i * blk:half, 0:half])
        slot(3)
        crosses(parity)
        for i in range(parts):
            sq = qacc[rows_at(i), i * blk:] + dot_nt(a[rows_at(i), half:], a[i * blk:half, half:])
            b[rows_at(i), i * blk:half] = poly(a[rows_at(i), i * blk:half], sq)
        slot(4)
        b[:, half:] = poly(a[0:half, half:], dot_nn(a[0:half, :], a[:, half:]))
        mirror(b, rows_at)
        a_drain(parity)
        for n, (left, width) in enumerate(tiles):
            slot(5 + n)
            cols = pl.ds(left, width)
            xn[0:half, cols] = renew(x[0:half, cols], dot_nn(b[...], x[:, cols]))
            x_copy(1 - parity, n).start()

    def ns_pair(pair, carry):
        ns_step(pair, 0)
        ns_step(pair, 1)
        return carry

    lax.fori_loop(0, NS_STEPS // 2, ns_pair, 0)

    def last_slot(s):
        for fn in tasks.get((NS_STEPS - 1, s), []):
            fn()

    grams(0, last_slot, lambda: x_wait(0))
    last_slot(3)
    crosses(0)
    a = grids[0]
    top = pl.ds(0, sc['own'][0].shape[1])
    b[top, 0:half] = poly(a[top, 0:half], dot_nt(a[top, :], a[0:half, :]))
    b[top, half:] = poly(a[top, half:], dot_nn(a[top, :], a[:, half:]))
    a_drain(0)
    sc['oa'][...] = renew(xs[0][top, :], dot_nn(b[top, :], xs[0][...]))
    out_copy(0, 1, sc['oa']).start()
    last_slot(4)

    for k in (1, 2):
        gath[k].finish()
        gath[k].drain()
    bu = sc['bu']
    up_rows, down_rows = sc['own'][1].shape[1], sc['own'][2].shape[1]
    up_send, down_send = sc['up_send'], sc['down_send']
    up_copy = remote(up_send, sc['ou'], sc['osend'].at[0], sc['orecv'].at[0], place.partner)
    down_copy = remote(down_send, sc['od'], sc['osend'].at[1], sc['orecv'].at[1], place.partner)
    half_wide = wide // 2

    @pl.when(core == 0)
    def _():
        def step(it, carry):
            bu[0] = dot_tn(tall[...], tall[...]).astype(BF16)
            bu[1] = poly(bu[0], dot_nn(bu[0], bu[0]))
            for n in (0, 1):
                rows = pl.ds(n * half_wide, half_wide)
                tall[rows, :] = renew(tall[rows, :], dot_nn(tall[rows, :], bu[1]))
            return carry
        lax.fori_loop(0, NS_STEPS - 1, step, 0)
        bu[0] = dot_tn(tall[...], tall[...]).astype(BF16)
        bu[1] = poly(bu[0], dot_nn(bu[0], bu[0]))
        other = tall[half_wide:half_wide + up_rows, :]
        up_send[...] = renew(other, dot_nn(other, bu[1]))
        up_copy.start()
        own = tall[0:up_rows, :]
        sc['ou'][...] = renew(own, dot_nn(own, bu[1]))
        out_copy(1, 1, sc['ou']).start()
        down_copy.wait_recv()
        out_copy(2, 1, sc['od']).start()
        up_copy.wait_send()

    @pl.when(core == 1)
    def _():
        def step(it, carry):
            bu[0] = dot_nt(xd[...], xd[...]).astype(BF16)
            bu[1] = poly(bu[0], dot_nn(bu[0], bu[0]))
            for n in (0, 1):
                cols = pl.ds(n * half_wide, half_wide)
                xd[:, cols] = renew(xd[:, cols], dot_nn(bu[1], xd[:, cols]))
            return carry
        lax.fori_loop(0, NS_STEPS - 1, step, 0)
        bu[0] = dot_nt(xd[...], xd[...]).astype(BF16)

        def rows_of(which):
            rows = pl.ds(which * (small // 2), down_rows)
            part = poly(bu[0, rows, :], dot_nn(bu[0, rows, :], bu[0]))
            return renew(xd[rows, :], dot_nn(part, xd[...]))
        down_send[...] = rows_of(1)
        down_copy.start()
        sc['od'][...] = rows_of(0)
        out_copy(2, 1, sc['od']).start()
        up_copy.wait_recv()
        out_copy(1, 1, sc['ou']).start()
        down_copy.wait_send()

    for k in range(3):
        scat[k].drain()
    norm_drain(0)
    norm_drain(1)
    for k in range(3):
        out_copy(k, 0, sc['mom'][k]).wait()
        out_copy(k, 1, sc[('oa', 'ou', 'od')[k]]).wait()


def results_kernel(scales, *refs):
    for k in range(3):
        mom, ortho, master = refs[k], refs[3 + k], refs[6 + k]
        mom_out, master_out, weight_out = refs[9 + 3 * k:12 + 3 * k]
        mom_out[...] = mom[...]
        old = master[...]
        new = old - LEARN_RATE * (scales[k] * ortho[...].astype(F32) + WEIGHT_DECAY * old)
        master_out[...] = new
        weight_out[...] = new.astype(BF16)


def solution(mesh):
    group = mesh.shape['data']
    chips = group // 2
    pieces = chips - 1
    grad_spec = P(('stage', 'data'), None, None, None)
    row_spec = P('stage', 'data', None)

    def step_local(*arrays):
        grads = [arrays[3 * k].reshape(arrays[3 * k].shape[2:]) for k in range(3)]
        moms = [arrays[3 * k + 1].reshape(arrays[3 * k + 1].shape[1:]) for k in range(3)]
        masters = [arrays[3 * k + 2].reshape(arrays[3 * k + 2].shape[1:]) for k in range(3)]
        shapes = [m.shape for m in moms]
        size = grads[0].shape[0]
        wide, small = grads[1].shape
        dma = pltpu.SemaphoreType.DMA
        names, scratch = [], []

        def add(name, item):
            names.append(name)
            scratch.append(item)

        for k, (rows, cols) in enumerate(shapes):
            add(('own', k), pltpu.VMEM((chips, rows, cols), F32))
            add(('pair', k), pltpu.VMEM((chips, rows, cols), F32))
            add(('ring', k), pltpu.VMEM((2, chips // 2, rows, cols), F32))
            add(('mom', k), pltpu.VMEM((rows, cols), F32))
        half = size // 2
        add(('x', 0), pltpu.VMEM((size, size), BF16))
        add(('x', 1), pltpu.VMEM((size, size), BF16))
        add(('a', 0), pltpu.VMEM((size, size), BF16))
        add(('a', 1), pltpu.VMEM((size, size), BF16))
        add('qacc', pltpu.VMEM((half, half), F32))
        add('b', pltpu.VMEM((half, size), BF16))
        add('ar', pltpu.VMEM((3, half // 3, half // 3), BF16))
        add('tall', pltpu.VMEM((wide, small), BF16))
        add('xd', pltpu.VMEM((small, wide), BF16))
        add('bu', pltpu.VMEM((2, small, small), BF16))
        for name, k in (('oa', 0), ('ou', 1), ('od', 2), ('up_send', 1), ('down_send', 2)):
            add(name, pltpu.VMEM(shapes[k], BF16))
        add(('norm', 0), pltpu.VMEM((group, 8, 128), F32))
        add(('norm', 1), pltpu.VMEM((group, 16, 128), F32))
        for name, shape in (('load', (3, chips)), ('psend', (3, chips)), ('precv', (3, chips)), ('rsend', (3, 2, pieces)), ('rrecv', (3, 2, pieces)),
                            ('gsend', (3, 2, pieces)), ('grecv', (3, 2, pieces)), ('fsend', (3, 2, chips)), ('frecv', (3, 2, chips)),
                            ('nsend', (2, group)), ('nrecv', (2, group)), ('insem', (3,)), ('outsem', (6,)), ('asend', (2, 6)), ('arecv', (2, 6)),
                            ('xsend', (3,)), ('xrecv', (3,)), ('osend', (2,)), ('orecv', (2,))):
            add(name, dma(shape))

        def body(*refs):
            sc = {}
            for name, ref in zip(names, refs[12:]):
                if isinstance(name, tuple):
                    sc.setdefault(name[0], []).append(ref)
                else:
                    sc[name] = ref
            kernel(group, refs[0:3], refs[3:6], refs[6:12], sc)

        anywhere = pl.BlockSpec(memory_space=pl.ANY)
        part_shape = []
        for shape in shapes:
            part_shape += [jax.ShapeDtypeStruct(shape, F32), jax.ShapeDtypeStruct(shape, BF16)]
        parts = pl.pallas_call(
            body,
            out_shape=tuple(part_shape),
            in_specs=[anywhere] * 6,
            out_specs=tuple([anywhere] * 6),
            scratch_shapes=scratch,
            compiler_params=pltpu.CompilerParams(collective_id=0, has_side_effects=True, vmem_limit_bytes=64 * 1024 * 1024 - 65536),
            name='muon',
        )(*grads, *moms)
        scales = [0.2 * math.sqrt(max(g.shape)) for g in grads]
        out_shape = []
        for shape in shapes:
            out_shape += [jax.ShapeDtypeStruct(shape, F32), jax.ShapeDtypeStruct(shape, F32), jax.ShapeDtypeStruct(shape, BF16)]
        vmem = pl.BlockSpec(memory_space=pltpu.VMEM)
        results = pl.pallas_call(
            functools.partial(results_kernel, scales),
            out_shape=tuple(out_shape),
            in_specs=[vmem] * 9,
            out_specs=tuple([vmem] * 9),
            name='results',
        )(*parts[0::2], *parts[1::2], *masters)
        return tuple(r[None] for r in results)

    in_specs = (grad_spec, row_spec, row_spec) * 3
    out_specs = (row_spec,) * 9
    return jax.shard_map(step_local, mesh=mesh, in_specs=in_specs, out_specs=out_specs, check_vma=False)
```

```python
import functools
import math
import jax
import jax.numpy as jnp
from jax import lax
from jax.experimental import pallas as pl
from jax.experimental.pallas import tpu as pltpu
from jax.sharding import PartitionSpec as P

MOMENTUM = 0.95
LEARN_RATE = 0.25
WEIGHT_DECAY = 0.2
EPSILON = 1e-7
COEF_A = 3.4445
COEF_B = -4.7750
COEF_C = 2.0315
NS_STEPS = 5
F32 = jnp.float32
BF16 = jnp.bfloat16


def dot_nn(a, b):
    return lax.dot_general(a, b, (((1,), (0,)), ((), ())), preferred_element_type=F32)


def dot_tn(a, b):
    return lax.dot_general(a, b, (((0,), (0,)), ((), ())), preferred_element_type=F32)


def dot_nt(a, b):
    return lax.dot_general(a, b, (((1,), (1,)), ((), ())), preferred_element_type=F32)


def remote(src, dst, send_sem, recv_sem, dev):
    return pltpu.make_async_remote_copy(
        src_ref=src, dst_ref=dst, send_sem=send_sem, recv_sem=recv_sem,
        device_id={'data': dev}, device_id_type=pl.DeviceIdType.MESH)


def ds(start, size, mult):
    return pl.ds(pl.multiple_of(start, mult), size)


class Place:
    def __init__(self, group):
        self.group = group
        self.chips = group // 2
        self.me = lax.axis_index('data')
        self.chip = self.me // 2
        self.core = self.me % 2
        self.partner = self.chip * 2 + (1 - self.core)

    def at(self, offset):
        return lax.rem(self.chip + offset + self.chips, self.chips)

    def next(self, way):
        return self.at(1 if way == 0 else -1) * 2 + self.core


class Scatter:
    def __init__(self, place, grad, own, pair, ring, load, psend, precv, rsend, rrecv):
        self.pl, self.grad, self.own, self.pair, self.ring = place, grad, own, pair, ring
        self.load, self.psend, self.precv, self.rsend, self.rrecv = load, psend, precv, rsend, rrecv
        self.rows = own.shape[1]
        self.half_rows = self.rows // 2
        self.n = place.chips
        self.pieces = self.n - 1

    def order(self):
        far = self.n // 2
        order = [far]
        for d in range(far - 1, 0, -1):
            order += [d, self.n - d]
        return order + [0]

    def load_copy(self, d):
        row = (self.pl.at(d) * 2 + self.pl.core) * self.rows
        return pltpu.make_async_copy(self.grad.at[ds(row, self.rows, 32), :], self.own.at[d], self.load.at[d])

    def pair_copy(self, d):
        row = (self.pl.at(d) * 2 + (1 - self.pl.core)) * self.rows
        return remote(self.grad.at[ds(row, self.rows, 32), :], self.pair.at[d], self.psend.at[d], self.precv.at[d], self.pl.partner)

    def start(self):
        for d in self.order():
            self.pair_copy(d).start()
            self.load_copy(d).start()

    def arrive(self, d):
        self.load_copy(d).wait()
        self.pair_copy(d).wait_recv()

    def spot(self, way, q):
        dist = self.n // 2 - (q + 1) // 2
        half = way if q % 2 == 0 else 1 - way
        return dist, (dist if way == 0 else (self.n - dist) % self.n), pl.ds(half * self.half_rows, self.half_rows)

    def ring_copy(self, way, q):
        dist, d, rows = self.spot(way, q)
        return remote(self.own.at[d, rows, :], self.ring.at[way, dist - 1, rows, :], self.rsend.at[way, q], self.rrecv.at[way, q], self.pl.next(way))

    def step(self, q):
        for way in (0, 1):
            dist, d, rows = self.spot(way, q)
            if q % 2 == 1 or (q == 0 and way == 0):
                self.arrive(d)
            total = self.own[d, rows, :] + self.pair[d, rows, :]
            if q >= 2:
                self.ring_copy(way, q - 2).wait_recv()
                total = total + self.ring[way, dist, rows, :]
            self.own[d, rows, :] = total
            self.ring_copy(way, q).start()

    def total(self):
        self.arrive(0)
        for way in (0, 1):
            for q in (self.pieces - 2, self.pieces - 1):
                self.ring_copy(way, q).wait_recv()
        return (self.own[0] + self.pair[0]) + (self.ring[0, 0] + self.ring[1, 0])

    def drain(self):
        for d in range(self.n):
            self.pair_copy(d).wait_send()
        for way in (0, 1):
            for q in range(self.pieces):
                self.ring_copy(way, q).wait_send()


class Gather:
    def __init__(self, place, full, other, rows, to, rsend, rrecv, fsend, frecv):
        self.pl, self.full, self.other, self.rows, self.to = place, full, other, rows, to
        self.rsend, self.rrecv, self.fsend, self.frecv = rsend, rrecv, fsend, frecv
        self.half_rows = rows // 2
        self.n = place.chips
        self.pieces = self.n - 1

    def rows_of(self, way, q, lag):
        hop = q // 2 + lag
        slot = 0 if hop == 0 else min(2 * hop - 1 + way, self.n - 1)
        half = way if q % 2 == 0 else 1 - way
        return pl.ds(slot * self.rows + half * self.half_rows, self.half_rows)

    def ring_copy(self, way, q):
        return remote(self.full.at[self.rows_of(way, q, 0), :], self.full.at[self.rows_of(way, q, 1), :],
                      self.rsend.at[way, q], self.rrecv.at[way, q], self.pl.next(way))

    def forward(self, way, q):
        rows = self.rows_of(way, q, 1)
        return remote(self.full.at[rows, :], self.other.at[rows, :], self.fsend.at[way, q], self.frecv.at[way, q], self.pl.partner)

    def forward_own(self):
        rows = pl.ds(0, self.rows)
        return remote(self.full.at[rows, :], self.other.at[rows, :], self.fsend.at[0, self.pieces], self.frecv.at[0, self.pieces], self.pl.partner)

    def sending(self, fn):
        if self.to is None:
            fn()
        else:
            pl.when(self.pl.core != self.to)(fn)

    def step(self, q):
        if q == 0:
            for k in (0, 1):
                for way in (0, 1):
                    self.ring_copy(way, k).start()
            self.sending(lambda: self.forward_own().start())
        else:
            for way in (0, 1):
                self.ring_copy(way, q - 1).wait_recv()
                if q + 1 < self.pieces:
                    self.ring_copy(way, q + 1).start()

            def hand_on():
                for way in (0, 1):
                    self.forward(way, q - 1).start()
            self.sending(hand_on)

    def steps(self):
        return self.pieces + 1

    def finish(self):
        def run():
            self.forward_own().wait_recv()
            for way in (0, 1):
                for q in range(self.pieces):
                    self.forward(way, q).wait_recv()
        if self.to is None:
            run()
        else:
            pl.when(self.pl.core == self.to)(run)

    def drain(self):
        for way in (0, 1):
            for q in range(self.pieces):
                self.ring_copy(way, q).wait_send()

        def run():
            self.forward_own().wait_send()
            for way in (0, 1):
                for q in range(self.pieces):
                    self.forward(way, q).wait_send()
        self.sending(run)


def squares(mat):
    sq = mat * mat
    rows, cols = mat.shape
    acc = sq[0:8]
    for i in range(1, rows // 8):
        acc = acc + sq[8 * i:8 * i + 8]
    out = acc[:, 0:128]
    for j in range(1, cols // 128):
        out = out + acc[:, 128 * j:128 * j + 128]
    return out


def total_norm(ref, top):
    acc = ref[0, top:top + 8]
    for i in range(1, ref.shape[0]):
        acc = acc + ref[i, top:top + 8]
    total = jnp.sum(jnp.sum(acc, axis=1, keepdims=True), axis=0, keepdims=True)
    return jnp.sqrt(total) + EPSILON


def kernel(group, grads, moms, outs, sc):
    place = Place(group)
    core, chip = place.core, place.chip
    chips = place.chips
    pieces = chips - 1
    barrier = pltpu.get_barrier_semaphore()
    for dev in (place.partner, place.next(0), place.next(1)):
        pl.semaphore_signal(barrier, inc=1, device_id={'data': dev}, device_id_type=pl.DeviceIdType.MESH)
    pl.semaphore_wait(barrier, 3)

    scat = [Scatter(place, grads[k], sc['own'][k], sc['pair'][k], sc['ring'][k], sc['load'].at[k], sc['psend'].at[k], sc['precv'].at[k],
                    sc['rsend'].at[k], sc['rrecv'].at[k]) for k in range(3)]
    xs = sc['x']
    size = xs[0].shape[0]
    half = size // 2
    xd, tall = sc['xd'], sc['tall']
    small, wide = xd.shape
    fulls = [xs[0].at[pl.ds(0, half), :], tall.at[pl.ds(0, wide // 2), :], xd.at[pl.ds(0, small // 2), :]]
    others = [xs[0].at[pl.ds(half, half), :], tall.at[pl.ds(wide // 2, wide // 2), :], xd.at[pl.ds(small // 2, small // 2), :]]
    gath = [Gather(place, fulls[k], others[k], sc['own'][k].shape[1], (None, 0, 1)[k], sc['gsend'].at[k], sc['grecv'].at[k], sc['fsend'].at[k], sc['frecv'].at[k])
            for k in range(3)]

    scat[0].start()
    in_copies = []
    for k in range(3):
        in_copies.append(pltpu.make_async_copy(moms[k], sc['mom'][k], sc['insem'].at[k]))
        in_copies[k].start()
    scat[1].start()
    scat[2].start()

    def out_copy(k, j, ref):
        return pltpu.make_async_copy(ref, outs[2 * k + j], sc['outsem'].at[2 * k + j])

    def momentum(k):
        in_copies[k].wait()
        mat = MOMENTUM * sc['mom'][k][...] + scat[k].total() * (1.0 / group)
        sc['mom'][k][...] = mat
        out_copy(k, 0, sc['mom'][k]).start()
        return squares(mat)

    def norm_copy(idx, i):
        ref = sc['norm'][idx]
        dev = lax.rem(place.me + i, group)
        return remote(ref.at[0], ref.at[i], sc['nsend'].at[idx, i], sc['nrecv'].at[idx, i], dev)

    def norm_send(idx):
        for i in range(1, group):
            norm_copy(idx, i).start()

    def norm_wait(idx):
        for i in range(1, group):
            norm_copy(idx, i).wait_recv()

    def norm_drain(idx):
        for i in range(1, group):
            norm_copy(idx, i).wait_send()

    def write_x(k, norm):
        rows = sc['own'][k].shape[1]
        fulls[k][0:rows, :] = (sc['mom'][k][...] / norm).astype(BF16)

    for q in range(pieces):
        scat[0].step(q)
    sc['norm'][0][0] = momentum(0)
    norm_send(0)
    for q in (0, 1):
        for k in (1, 2):
            scat[k].step(q)
    norm_wait(0)
    write_x(0, total_norm(sc['norm'][0], 0))
    for q in range(gath[0].steps()):
        gath[0].step(q)
        if q + 2 == pieces:
            for k in (1, 2):
                scat[k].step(2)

    tasks = {}

    def background(it, slot, fn):
        tasks.setdefault((it, slot), []).append(fn)

    def ud_momentum():
        sc['norm'][1][0, 0:8] = momentum(1)
        sc['norm'][1][0, 8:16] = momentum(2)
        norm_send(1)

    def ud_write():
        norm_wait(1)
        write_x(1, total_norm(sc['norm'][1], 0))
        write_x(2, total_norm(sc['norm'][1], 8))

    def both(parts, q):
        def run():
            parts[1].step(q)
            parts[2].step(q)
        return run

    background(0, 0, both(scat, 3))
    for q, place_at in ((4, (0, 3)), (5, (0, 6)), (6, (1, 2))):
        background(*place_at, both(scat, q))
    background(1, 7, ud_momentum)
    background(2, 4, ud_write)
    times = ((2, 4), (2, 7), (3, 1), (3, 3), (3, 5), (3, 7), (4, 1), (4, 3))
    for q in range(gath[1].steps()):
        background(*times[q], both(gath, q))

    grids, b, ar, qacc = sc['a'], sc['b'], sc['ar'], sc['qacc']
    parts = 3
    blk = half // parts
    tiles = tuple((n * 2 * blk, 2 * blk) for n in range(parts))

    def rows_at(i):
        return pl.ds(i * blk, blk)

    def far_at(i):
        return pl.ds(half + i * blk, blk)

    def cross_copy(way, t):
        return remote(grids[way].at[rows_at(t), far_at((t + 1) % parts)], ar.at[t], sc['asend'].at[way, t], sc['arecv'].at[way, t], place.partner)

    def own_copy(way, i):
        width = half - i * blk
        return remote(grids[way].at[rows_at(i), pl.ds(i * blk, width)], grids[way].at[far_at(i), pl.ds(half + i * blk, width)],
                      sc['asend'].at[way, parts + i], sc['arecv'].at[way, parts + i], place.partner)

    def x_copy(way, n):
        cols = pl.ds(*tiles[n])
        return remote(xs[way].at[pl.ds(0, half), cols], xs[way].at[pl.ds(half, half), cols], sc['xsend'].at[n], sc['xrecv'].at[n], place.partner)

    def x_wait(way):
        for n in range(len(tiles)):
            x_copy(way, n).wait_recv()
            x_copy(way, n).wait_send()

    def mirror(ref, at):
        for i in range(parts):
            for j in range(i + 1, parts):
                ref[at(j), at(i)] = ref[at(i), at(j)].T

    def grams(way, slot, wait):
        x, a = xs[way], grids[way]
        slot(0)
        for i in range(parts):
            a[rows_at(i), i * blk:half] = dot_nt(x[rows_at(i), :], x[i * blk:half, :]).astype(BF16)
        for i in range(parts):
            own_copy(way, i).start()
        slot(1)
        wait()
        for t in range(parts):
            a[rows_at(t), far_at((t + 1) % parts)] = dot_nt(x[rows_at(t), :], x[far_at((t + 1) % parts), :]).astype(BF16)
        for t in range(parts):
            cross_copy(way, t).start()
        slot(2)
        mirror(a, rows_at)
        for t in range(parts):
            a[rows_at(t), far_at(t)] = dot_nt(x[rows_at(t), :], x[far_at(t), :]).astype(BF16)

    def crosses(way):
        a = grids[way]
        for t in range(parts):
            own_copy(way, t).wait_recv()
            cross_copy(way, t).wait_recv()
        for t in range(parts):
            a[rows_at((t + 1) % parts), far_at(t)] = ar[t].T
        mirror(a, far_at)

    def a_drain(way):
        for t in range(parts):
            own_copy(way, t).wait_send()
            cross_copy(way, t).wait_send()

    def poly(lin, acc):
        return (COEF_B * lin.astype(F32) + COEF_C * acc.astype(BF16).astype(F32)).astype(BF16)

    def renew(old, upd):
        return (COEF_A * old.astype(F32) + upd.astype(BF16).astype(F32)).astype(BF16)

    def ns_step(pair, parity):
        x, xn, a = xs[parity], xs[1 - parity], grids[parity]

        def slot(s):
            for (t, u), fns in tasks.items():
                if u == s and t % 2 == parity and t < NS_STEPS - 1:
                    def run(fns=fns):
                        for fn in fns:
                            fn()
                    pl.when(pair == t // 2)(run)

        def wait():
            if parity == 0:
                @pl.when(pair == 0)
                def _():
                    gath[0].finish()
                    gath[0].drain()

                @pl.when(pair > 0)
                def _():
                    x_wait(0)
            else:
                x_wait(1)

        grams(parity, slot, wait)
        for i in range(parts):
            qacc[rows_at(i), i * blk:] = dot_nt(a[rows_at(i), 0:half], a[i * blk:half, 0:half])
        slot(3)
        crosses(parity)
        for i in range(parts):
            sq = qacc[rows_at(i), i * blk:] + dot_nt(a[rows_at(i), half:], a[i * blk:half, half:])
            b[rows_at(i), i * blk:half] = poly(a[rows_at(i), i * blk:half], sq)
        slot(4)
        b[:, half:] = poly(a[0:half, half:], dot_nn(a[0:half, :], a[:, half:]))
        mirror(b, rows_at)
        a_drain(parity)
        for n, (left, width) in enumerate(tiles):
            slot(5 + n)
            cols = pl.ds(left, width)
            xn[0:half, cols] = renew(x[0:half, cols], dot_nn(b[...], x[:, cols]))
            x_copy(1 - parity, n).start()

    def ns_pair(pair, carry):
        ns_step(pair, 0)
        ns_step(pair, 1)
        return carry

    lax.fori_loop(0, NS_STEPS // 2, ns_pair, 0)

    def last_slot(s):
        for fn in tasks.get((NS_STEPS - 1, s), []):
            fn()

    grams(0, last_slot, lambda: x_wait(0))
    last_slot(3)
    crosses(0)
    a = grids[0]
    top = pl.ds(0, sc['own'][0].shape[1])
    b[top, 0:half] = poly(a[top, 0:half], dot_nt(a[top, :], a[0:half, :]))
    b[top, half:] = poly(a[top, half:], dot_nn(a[top, :], a[:, half:]))
    a_drain(0)
    sc['oa'][...] = renew(xs[0][top, :], dot_nn(b[top, :], xs[0][...]))
    out_copy(0, 1, sc['oa']).start()
    last_slot(4)

    for k in (1, 2):
        gath[k].finish()
        gath[k].drain()
    bu = sc['bu']
    up_rows, down_rows = sc['own'][1].shape[1], sc['own'][2].shape[1]
    up_send, down_send = sc['up_send'], sc['down_send']
    up_copy = remote(up_send, sc['ou'], sc['osend'].at[0], sc['orecv'].at[0], place.partner)
    down_copy = remote(down_send, sc['od'], sc['osend'].at[1], sc['orecv'].at[1], place.partner)
    half_wide = wide // 2

    @pl.when(core == 0)
    def _():
        def step(it, carry):
            bu[0] = dot_tn(tall[...], tall[...]).astype(BF16)
            bu[1] = poly(bu[0], dot_nn(bu[0], bu[0]))
            for n in (0, 1):
                rows = pl.ds(n * half_wide, half_wide)
                tall[rows, :] = renew(tall[rows, :], dot_nn(tall[rows, :], bu[1]))
            return carry
        lax.fori_loop(0, NS_STEPS - 1, step, 0)
        bu[0] = dot_tn(tall[...], tall[...]).astype(BF16)
        bu[1] = poly(bu[0], dot_nn(bu[0], bu[0]))
        other = tall[half_wide:half_wide + up_rows, :]
        up_send[...] = renew(other, dot_nn(other, bu[1]))
        up_copy.start()
        own = tall[0:up_rows, :]
        sc['ou'][...] = renew(own, dot_nn(own, bu[1]))
        out_copy(1, 1, sc['ou']).start()
        down_copy.wait_recv()
        out_copy(2, 1, sc['od']).start()
        up_copy.wait_send()

    @pl.when(core == 1)
    def _():
        def step(it, carry):
            bu[0] = dot_nt(xd[...], xd[...]).astype(BF16)
            bu[1] = poly(bu[0], dot_nn(bu[0], bu[0]))
            for n in (0, 1):
                cols = pl.ds(n * half_wide, half_wide)
                xd[:, cols] = renew(xd[:, cols], dot_nn(bu[1], xd[:, cols]))
            return carry
        lax.fori_loop(0, NS_STEPS - 1, step, 0)
        bu[0] = dot_nt(xd[...], xd[...]).astype(BF16)

        def rows_of(which):
            rows = pl.ds(which * (small // 2), down_rows)
            part = poly(bu[0, rows, :], dot_nn(bu[0, rows, :], bu[0]))
            return renew(xd[rows, :], dot_nn(part, xd[...]))
        down_send[...] = rows_of(1)
        down_copy.start()
        sc['od'][...] = rows_of(0)
        out_copy(2, 1, sc['od']).start()
        up_copy.wait_recv()
        out_copy(1, 1, sc['ou']).start()
        down_copy.wait_send()

    for k in range(3):
        scat[k].drain()
    norm_drain(0)
    norm_drain(1)
    for k in range(3):
        out_copy(k, 0, sc['mom'][k]).wait()
        out_copy(k, 1, sc[('oa', 'ou', 'od')[k]]).wait()


def results_kernel(scales, *refs):
    for k in range(3):
        mom, ortho, master = refs[k], refs[3 + k], refs[6 + k]
        mom_out, master_out, weight_out = refs[9 + 3 * k:12 + 3 * k]
        mom_out[...] = mom[...]
        old = master[...]
        new = old - LEARN_RATE * (scales[k] * ortho[...].astype(F32) + WEIGHT_DECAY * old)
        master_out[...] = new
        weight_out[...] = new.astype(BF16)


def solution(mesh):
    group = mesh.shape['data']
    chips = group // 2
    pieces = chips - 1
    grad_spec = P(('stage', 'data'), None, None, None)
    row_spec = P('stage', 'data', None)

    def step_local(*arrays):
        grads = [arrays[3 * k].reshape(arrays[3 * k].shape[2:]) for k in range(3)]
        moms = [arrays[3 * k + 1].reshape(arrays[3 * k + 1].shape[1:]) for k in range(3)]
        masters = [arrays[3 * k + 2].reshape(arrays[3 * k + 2].shape[1:]) for k in range(3)]
        shapes = [m.shape for m in moms]
        size = grads[0].shape[0]
        wide, small = grads[1].shape
        dma = pltpu.SemaphoreType.DMA
        names, scratch = [], []

        def add(name, item):
            names.append(name)
            scratch.append(item)

        for k, (rows, cols) in enumerate(shapes):
            add(('own', k), pltpu.VMEM((chips, rows, cols), F32))
            add(('pair', k), pltpu.VMEM((chips, rows, cols), F32))
            add(('ring', k), pltpu.VMEM((2, chips // 2, rows, cols), F32))
            add(('mom', k), pltpu.VMEM((rows, cols), F32))
        half = size // 2
        add(('x', 0), pltpu.VMEM((size, size), BF16))
        add(('x', 1), pltpu.VMEM((size, size), BF16))
        add(('a', 0), pltpu.VMEM((size, size), BF16))
        add(('a', 1), pltpu.VMEM((size, size), BF16))
        add('qacc', pltpu.VMEM((half, half), F32))
        add('b', pltpu.VMEM((half, size), BF16))
        add('ar', pltpu.VMEM((3, half // 3, half // 3), BF16))
        add('tall', pltpu.VMEM((wide, small), BF16))
        add('xd', pltpu.VMEM((small, wide), BF16))
        add('bu', pltpu.VMEM((2, small, small), BF16))
        for name, k in (('oa', 0), ('ou', 1), ('od', 2), ('up_send', 1), ('down_send', 2)):
            add(name, pltpu.VMEM(shapes[k], BF16))
        add(('norm', 0), pltpu.VMEM((group, 8, 128), F32))
        add(('norm', 1), pltpu.VMEM((group, 16, 128), F32))
        for name, shape in (('load', (3, chips)), ('psend', (3, chips)), ('precv', (3, chips)), ('rsend', (3, 2, pieces)), ('rrecv', (3, 2, pieces)),
                            ('gsend', (3, 2, pieces)), ('grecv', (3, 2, pieces)), ('fsend', (3, 2, chips)), ('frecv', (3, 2, chips)),
                            ('nsend', (2, group)), ('nrecv', (2, group)), ('insem', (3,)), ('outsem', (6,)), ('asend', (2, 6)), ('arecv', (2, 6)),
                            ('xsend', (3,)), ('xrecv', (3,)), ('osend', (2,)), ('orecv', (2,))):
            add(name, dma(shape))

        def body(*refs):
            sc = {}
            for name, ref in zip(names, refs[12:]):
                if isinstance(name, tuple):
                    sc.setdefault(name[0], []).append(ref)
                else:
                    sc[name] = ref
            kernel(group, refs[0:3], refs[3:6], refs[6:12], sc)

        anywhere = pl.BlockSpec(memory_space=pl.ANY)
        part_shape = []
        for shape in shapes:
            part_shape += [jax.ShapeDtypeStruct(shape, F32), jax.ShapeDtypeStruct(shape, BF16)]
        parts = pl.pallas_call(
            body,
            out_shape=tuple(part_shape),
            in_specs=[anywhere] * 6,
            out_specs=tuple([anywhere] * 6),
            scratch_shapes=scratch,
            compiler_params=pltpu.CompilerParams(collective_id=0, has_side_effects=True, vmem_limit_bytes=64 * 1024 * 1024 - 65536),
            name='muon',
        )(*grads, *moms)
        scales = [0.2 * math.sqrt(max(g.shape)) for g in grads]
        out_shape = []
        for shape in shapes:
            out_shape += [jax.ShapeDtypeStruct(shape, F32), jax.ShapeDtypeStruct(shape, F32), jax.ShapeDtypeStruct(shape, BF16)]
        vmem = pl.BlockSpec(memory_space=pltpu.VMEM)
        results = pl.pallas_call(
            functools.partial(results_kernel, scales),
            out_shape=tuple(out_shape),
            in_specs=[vmem] * 9,
            out_specs=tuple([vmem] * 9),
            name='results',
        )(*parts[0::2], *parts[1::2], *masters)
        return tuple(r[None] for r in results)

    in_specs = (grad_spec, row_spec, row_spec) * 3
    out_specs = (row_spec,) * 9
    return jax.shard_map(step_local, mesh=mesh, in_specs=in_specs, out_specs=out_specs, check_vma=False)
```
